512 devices in a mesh: dp: 32 (over y_hi, x, core), mp: 16 (over y_lo, z).
Axes of the slice: x: 4, y: 8 (y_hi: 4, y_lo: 2; y = y_hi * 2 + y_lo), z: 8, core: 2. Of those that a mesh axis runs over, the one named last changes fastest.
Arguments:
- activations: bfloat16 [32, 128, 4096], P('dp', None, 'mp'), may hold values from -6 to 6
- gradients: bfloat16 [32, 128, 11008], P('dp', None, 'mp'), may hold values from -12 to 12, as said below
- basis_in: bfloat16 [4096, 4096], P(None, 'mp'), may hold values from -0.09375 to 0.09375
- basis_out: bfloat16 [11008, 11008], P('mp', 'dp'), may hold values from -0.0546875 to 0.0546875
Outputs:
- eigen_diag: float32 [11008, 4096], P('dp', 'mp')
The draws below stay inside these ranges and needn't reach their ends.
Inputs may be any that keep to these rules, and one draw needn't show every extreme that they name: `gradients`: gradients are real-valued with varying scales.
All inputs are finite; a program needn't handle non-finite values.
Results may differ from the reference program's by a relative error of at most 0.02.
Values may be sent and summed in bfloat16 or wider, within the bound.
A program may use at most 64 MiB of HBM per device.

```python
import jax
import jax.numpy as jnp
from jax import lax

D_IN = 4096
D_OUT = 11008
SEQ_LEN = 128
SEQS = 32
N_MP = 16


def draw_gradients(key, part):
    key_base = jax.random.fold_in(jax.random.fold_in(key, 7), 0)
    key_jitter = jax.random.fold_in(jax.random.fold_in(key, 7), 2)
    key_token = jax.random.fold_in(jax.random.fold_in(key, 7), 3)
    base = jax.random.normal(key_base, (SEQS, SEQ_LEN, D_OUT), jnp.float32)
    position = jnp.arange(SEQS, dtype=jnp.float32) / max(SEQS - 1, 1)
    jitter = jax.random.uniform(key_jitter, (SEQS,), jnp.float32, 0.8, 1.25)
    seq_scale = (1.0 + 2.0 * position) * jitter
    token_scale = jnp.exp(jax.random.uniform(key_token, (SEQS, SEQ_LEN, 1), jnp.float32, -0.5, 0.5))
    values = base * seq_scale[:, None, None] * token_scale * 0.6
    return jnp.clip(values, -12.0, 12.0).astype(jnp.bfloat16)


def steps_of(key, extent, cuts, smallest, largest):
    factor_of = 1.0
    for dim, blocks in cuts:
        steps = jax.random.uniform(jax.random.fold_in(jax.random.fold_in(key, 6), dim), (blocks,), jnp.float32, smallest / len(cuts), largest / len(cuts))
        factor_of = factor_of * jnp.repeat(jnp.exp(steps), extent[dim] // blocks).reshape((-1,) + (1,) * (len(extent) - 1 - dim))
    return factor_of


def normal_values(rng, dims, spread, bound, cuts=(), kind=jnp.bfloat16):
    entries = spread * jax.random.normal(rng, dims, jnp.float32)
    if cuts:
        entries = entries * steps_of(rng, dims, cuts, -0.22, 0.18)
    return jnp.clip(entries, -bound, bound).astype(kind)


def setup_inputs(seed: int = 0) -> dict:
    splits = jax.random.split(jax.random.key(seed), 5)
    activations = normal_values(splits[0], (SEQS, SEQ_LEN, D_IN), 1.0, 6.0, ((0, 32), (2, 16)))
    gradients = draw_gradients(jax.random.fold_in(splits[4], 71), 0)
    basis_in = normal_values(splits[2], (D_IN, D_IN), D_IN ** -0.5, 0.09375, ((1, 16),))
    basis_out = normal_values(splits[3], (D_OUT, D_OUT), D_OUT ** -0.5, 0.0546875, ((0, 16), (1, 32)))
    return {"activations": activations, "gradients": gradients, "basis_in": basis_in, "basis_out": basis_out}


def reference(activations, gradients, basis_in, basis_out):
    block_width = D_OUT // N_MP
    grad_rows = gradients.reshape(SEQS * SEQ_LEN, D_OUT).astype(jnp.float32)
    basis_rows = basis_out.astype(jnp.float32)
    summed = jnp.zeros((SEQS * SEQ_LEN, D_OUT), jnp.float32)
    for block in range(N_MP):
        lower = block * block_width
        part_term = jnp.dot(grad_rows[:, lower:lower + block_width], basis_rows[lower:lower + block_width, :])
        rounded = lax.optimization_barrier(part_term.astype(jnp.bfloat16))
        summed = summed + rounded.astype(jnp.float32)
    proj_grad = summed.astype(jnp.bfloat16).reshape(SEQS, SEQ_LEN, D_OUT)
    act_rows = activations.reshape(SEQS * SEQ_LEN, D_IN).astype(jnp.float32)
    proj_act = jnp.dot(act_rows, basis_in.astype(jnp.float32)).astype(jnp.bfloat16).reshape(SEQS, SEQ_LEN, D_IN)

    def accumulate(carry, pair):
        grad_seq, act_seq = pair
        seq_grad = jnp.dot(grad_seq.astype(jnp.float32).T, act_seq.astype(jnp.float32))
        return carry + seq_grad * seq_grad, None

    start_carry = jnp.zeros((D_OUT, D_IN), jnp.float32)
    squares, _ = lax.scan(accumulate, start_carry, (proj_grad, proj_act))
    return squares * (1.0 / (SEQS * SEQ_LEN))
```

```python
import functools

import jax
import jax.numpy as jnp
from jax import lax
from jax.experimental import pallas as pl
from jax.experimental.pallas import tpu as pltpu
from jax.sharding import PartitionSpec as P

MESH = pl.DeviceIdType.MESH
NX, NYH, NYL, NZ = 4, 4, 2, 8
F32, BF16 = jnp.float32, jnp.bfloat16


def kernel(
    dims, gt_ref, bt_ref, act_ref, bin_hbm, out_ref,
    bt, g, act, binv, paloc, pa, part, rsb, pg, acc, xrecv, ysend, yrecv,
    send_sems, recv_sems,
):
    feat, seq, half, chunk, width = dims
    dp, mp = lax.axis_index("dp"), lax.axis_index("mp")
    core, x, yh = dp % 2, (dp // 2) % NX, dp // (2 * NX)
    yl, z = mp // NZ, mp % NZ

    def dev(yh_=None, x_=None, c_=None, yl_=None, z_=None):
        yh_ = yh if yh_ is None else yh_
        x_ = x if x_ is None else x_
        c_ = core if c_ is None else c_
        yl_ = yl if yl_ is None else yl_
        z_ = z if z_ is None else z_
        return ((yh_ * NX + x_) * 2 + c_, yl_ * NZ + z_)

    sibling = dev(c_=1 - core)
    ypart = dev(yl_=1 - yl)
    xn = {1: dev(x_=(x + 1) % NX), -1: dev(x_=(x + NX - 1) % NX)}
    zn = {1: dev(z_=(z + 1) % NZ), -1: dev(z_=(z + NZ - 1) % NZ)}

    barrier = pltpu.get_barrier_semaphore()
    peers = [sibling, xn[1], xn[-1], zn[1], zn[-1]]
    y = yh * NYL + yl
    for k in range(1, NYH * NYL):
        yy = (y + k) % (NYH * NYL)
        peers.append(dev(yh_=yy // NYL, yl_=yy % NYL))
    for peer in peers:
        pl.semaphore_signal(barrier, inc=1, device_id=peer, device_id_type=MESH)
    pl.semaphore_wait(barrier, len(peers))

    counter = [0]
    sent = []

    def take(n=1):
        base = counter[0]
        counter[0] += n
        return base

    def send(src, dst, ssem, rsem, to):
        copy = pltpu.make_async_remote_copy(
            src_ref=src, dst_ref=dst, send_sem=send_sems.at[ssem], recv_sem=recv_sems.at[rsem],
            device_id=to, device_id_type=MESH,
        )
        copy.start()
        sent.append(copy)

    def arrived(dst, rsem):
        pltpu.make_async_copy(dst, dst, recv_sems.at[rsem]).wait()

    s_bt = take(3)
    s_act0 = take(1)
    s_gy, s_gx = take(4), take(16)
    s_py, s_px = take(4), take(16)
    s_actz = take(16)
    s_rs, s_ag = take(32), take(32)
    s_out = take(2)
    s_loc = take(3)

    hcls, aidx = yh % 2, yh // 2

    def y_start(src, place, sbase):
        for k in (1, 3, 2):
            send(src, place(0, aidx, yl), sbase + k, sbase + aidx * 2 + yl, dev(yh_=(yh + k) % NYH, yl_=hcls))

        def own():
            pltpu.make_async_copy(src, place(0, aidx, yl), recv_sems.at[sbase + aidx * 2 + yl]).start()

        def other():
            pltpu.make_async_remote_copy(
                src_ref=src, dst_ref=place(0, aidx, yl), send_sem=send_sems.at[sbase],
                recv_sem=recv_sems.at[sbase + aidx * 2 + yl], device_id=ypart, device_id_type=MESH,
            ).start()

        pl.when(yl == hcls)(own)
        pl.when(yl != hcls)(other)

    def y_finish(src, place, sbase):
        def other():
            pltpu.make_async_remote_copy(
                src_ref=src, dst_ref=place(0, aidx, yl), send_sem=send_sems.at[sbase],
                recv_sem=recv_sems.at[sbase + aidx * 2 + yl], device_id=ypart, device_id_type=MESH,
            ).wait_send()

        pl.when(yl != hcls)(other)

    def y_to_x(place, sbase, xbase, a, f):
        arrived(place(0, a, f), sbase + a * 2 + f)
        for d, slot in ((1, 1), (-1, 2)):
            send(place(0, a, f), place(slot, a, f), xbase + slot * 4 + a * 2 + f, xbase + slot * 4 + a * 2 + f, xn[d])

    def x_near(place, xbase, a, f):
        for d, slot in ((1, 1), (-1, 2)):
            arrived(place(slot, a, f), xbase + slot * 4 + a * 2 + f)
            if f == slot - 1:
                send(place(slot, a, f), place(3, a, f), xbase + 12 + a * 2 + f, xbase + 12 + a * 2 + f, xn[d])

    def x_far(place, xbase, a, f):
        arrived(place(3, a, f), xbase + 12 + a * 2 + f)

    def g_place(slot, a, f):
        return g.at[slot, f, :, pl.ds(pl.multiple_of(a * seq, 128), seq)]

    def p_place(slot, a, f):
        return pa.at[slot, pl.ds(pl.multiple_of(a * seq, 16), seq), pl.ds(pl.multiple_of(f * width, 128), width)]

    def bt_place(f, c):
        return bt.at[f, pl.ds(pl.multiple_of(c * half, 16), half), :]

    def start():
        pltpu.make_async_copy(bin_hbm, binv, recv_sems.at[s_loc]).start()
        pltpu.make_async_copy(bt_ref, bt_place(yl, core), recv_sems.at[s_loc + 1]).start()
        pltpu.make_async_copy(act_ref, act.at[yl, z], recv_sems.at[s_loc + 2]).start()
        send(act_ref, act.at[yl, z], s_act0, s_act0, ypart)
        y_start(gt_ref, g_place, s_gy)
        send(bt_ref, bt_place(yl, core), s_bt, s_bt, sibling)
        send(bt_ref, bt_place(yl, core), s_bt + 1, s_bt + 1, ypart)

    def bt_forward():
        arrived(bt_place(1 - yl, core), s_bt + 1)
        send(bt_place(1 - yl, core), bt_place(1 - yl, core), s_bt + 2, s_bt + 2, sibling)

    def bt_ready():
        arrived(bt_place(yl, 1 - core), s_bt)
        arrived(bt_place(1 - yl, 1 - core), s_bt + 2)
        arrived(bt_place(yl, core), s_loc + 1)

    def reach(f, d):
        return 4 if (f == 0) == (d == 1) else 3

    def act_sem(f, d, k):
        return s_actz + f * 8 + (0 if d == 1 else 4) + k

    def act_first():
        arrived(act.at[1 - yl, z], s_act0)
        for d in (1, -1):
            send(act_ref, act.at[yl, z], act_sem(yl, d, 0), act_sem(yl, d, 0), zn[d])
            send(act.at[1 - yl, z], act.at[1 - yl, z], act_sem(1 - yl, d, 0), act_sem(1 - yl, d, 0), zn[d])

    def act_step(k):
        for f in range(2):
            for d in (1, -1):
                n = reach(f, d)
                if k <= n:
                    zz = (z + NZ - d * k) % NZ
                    arrived(act.at[f, zz], act_sem(f, d, k - 1))
                    if k < n:
                        send(act.at[f, zz], act.at[f, zz], act_sem(f, d, k), act_sem(f, d, k), zn[d])

    def project_acts():
        arrived(act.at[yl, z], s_loc + 2)
        arrived(binv, s_loc)

        def body(i, total):
            rows = pl.ds(pl.multiple_of(i * width, 128), width)
            return total + jnp.dot(act[i // NZ, i % NZ], binv[rows, :], preferred_element_type=F32)

        total = lax.fori_loop(0, NYL * NZ, body, jnp.zeros((seq, width), F32))
        paloc[...] = total.astype(BF16)

    def project(grp):
        def body(r, carry):
            rows = pl.ds(pl.multiple_of(r * chunk, 16), chunk)
            t = jnp.dot(bt[0, rows, :], g[grp, 0], preferred_element_type=F32)
            t = t + jnp.dot(bt[1, rows, :], g[grp, 1], preferred_element_type=F32)
            t = t.astype(BF16)
            part[grp, r] = t[:, :seq]
            part[grp, r + 4] = t[:, seq:]
            return carry

        lax.fori_loop(0, 4, body, 0)

    def rlen(grp, d):
        return 4 if (grp % 2 == 0) == (d == 1) else 3

    def rs_slot(d, k):
        return (0 if d == 1 else 4) + k

    def rs_step(grp, k):
        for d in (1, -1):
            n = rlen(grp, d)
            if k < n:
                j = (z + NZ + d * (n - k)) % NZ
                if k == 0:
                    src = part.at[grp, j]
                else:
                    slot = rs_slot(d, k - 1)
                    src = rsb.at[grp, slot]
                    arrived(src, s_rs + grp * 8 + slot)
                    rsb[grp, slot] = (rsb[grp, slot].astype(F32) + part[grp, j].astype(F32)).astype(BF16)
                s = s_rs + grp * 8 + rs_slot(d, k)
                send(src, rsb.at[grp, rs_slot(d, k)], s, s, zn[d])

    def pg_place(grp, j):
        return pg.at[grp, pl.ds(pl.multiple_of(j * chunk, 16), chunk), :]

    def ag_sem(grp, d, k):
        return s_ag + grp * 8 + rs_slot(d, k)

    def rs_last(grp):
        total = part[grp, z].astype(F32)
        for d in (1, -1):
            slot = rs_slot(d, rlen(grp, d) - 1)
            arrived(rsb.at[grp, slot], s_rs + grp * 8 + slot)
            total = total + rsb[grp, slot].astype(F32)
        pg[grp, pl.ds(pl.multiple_of(z * chunk, 16), chunk), :] = total.astype(BF16)
        for d in (1, -1):
            send(pg_place(grp, z), pg_place(grp, z), ag_sem(grp, d, 0), ag_sem(grp, d, 0), zn[d])

    def ag_step(grp, k):
        for d in (1, -1):
            n = rlen(grp, d)
            if k <= n:
                j = (z + NZ - d * k) % NZ
                arrived(pg_place(grp, j), ag_sem(grp, d, k - 1))
                if k < n:
                    send(pg_place(grp, j), pg_place(grp, j), ag_sem(grp, d, k), ag_sem(grp, d, k), zn[d])

    def squares(grp, first):
        def body(r, carry):
            rows = pl.ds(pl.multiple_of(r * chunk, 16), chunk)
            total = None if first else acc[rows, :]
            for a in range(2):
                lhs = pg[grp, pl.ds(pl.multiple_of((a * 4 + r) * chunk, 16), chunk), :]
                t = jnp.dot(lhs, pa[grp, a * seq:(a + 1) * seq, :], preferred_element_type=F32)
                total = t * t if total is None else total + t * t
            acc[rows, :] = total
            return carry

        lax.fori_loop(0, 4, body, 0)

    def out_core():
        theirs = acc.at[pl.ds(pl.multiple_of((1 - core) * half, 8), half), :]
        send(theirs, xrecv, s_out, s_out, sibling)
        arrived(xrecv, s_out)

    def out_y():
        mine = pl.ds(pl.multiple_of(core * half, 8), half)
        away = pl.ds(pl.multiple_of((1 - yl) * width, 128), width)
        keep = pl.ds(pl.multiple_of(yl * width, 128), width)
        ysend[...] = (acc[mine, away] + xrecv[:, away]).astype(BF16)
        send(ysend, yrecv, s_out + 1, s_out + 1, ypart)
        xrecv[:, keep] = acc[mine, keep] + xrecv[:, keep]
        arrived(yrecv, s_out + 1)
        rows = out_ref.shape[0]
        out_ref[...] = (xrecv[:rows, keep] + yrecv[:rows, :].astype(F32)) * (1.0 / 4096.0)

    steps = []

    def at(t, fn, *args):
        steps.append((t, len(steps), functools.partial(fn, *args)))

    at(0, start)
    at(3, act_first)
    quads = [(0, 0), (0, 1), (1, 0), (1, 1)]
    for i, (a, f) in enumerate(quads):
        at(5 + 3 * i, y_to_x, g_place, s_gy, s_gx, a, f)
        at((18, 18.1, 21, 21.1)[i], x_near, g_place, s_gx, a, f)
        at(30, x_far, g_place, s_gx, a, f)
        at(24 + 0.1 * i, y_to_x, p_place, s_py, s_px, a, f)
        at(33 + 0.1 * i, x_near, p_place, s_px, a, f)
        at(43.9, x_far, p_place, s_px, a, f)
    for k, t in ((1, 7), (2, 11.5), (3, 14.5), (4, 17)):
        at(t, act_step, k)
    at(14.2, bt_forward)
    at(15, bt_ready)
    at(17.5, project_acts)
    at(17.6, y_start, paloc, p_place, s_py)
    for grp, t0, r0, a0 in ((0, 15.5, 19, 29), (1, 22, 26.1, 36), (2, 22.5, 26.2, 36.2), (3, 31, 34.5, 44)):
        at(t0, project, grp)
        at(t0 + 0.1, rs_step, grp, 0)
        for k in (1, 2, 3):
            at(r0 + 3.3 * (k - 1), rs_step, grp, k)
        at(a0, rs_last, grp)
        for k in (1, 2, 3, 4):
            at(a0 + 3 * k, ag_step, grp, k)
    at(44.5, squares, 0, True)
    at(49, squares, 1, False)
    at(49.5, squares, 2, False)
    at(57, squares, 3, False)
    at(60, out_core)
    at(61, out_y)
    for _, _, fn in sorted(steps, key=lambda s: (s[0], s[1])):
        fn()
    y_finish(gt_ref, g_place, s_gy)
    y_finish(paloc, p_place, s_py)
    for copy in sent:
        copy.wait_send()


def shards(activations, gradients, basis_in, basis_out):
    seq, feat = gradients.shape[1:]
    cols = basis_out.shape[1]
    width = basis_in.shape[1]
    half = (cols + 31) // 32 * 32
    chunk = half // 2
    gt = gradients[0].T
    bt = jnp.pad(basis_out.T, ((0, half - cols), (0, 0)))
    dims = (feat, seq, half, chunk, width)
    n_sems = 160
    return pl.pallas_call(
        functools.partial(kernel, dims),
        out_shape=jax.ShapeDtypeStruct((cols, width), F32),
        in_specs=[pl.BlockSpec(memory_space=pltpu.VMEM)] * 3 + [pl.BlockSpec(memory_space=pl.ANY)],
        out_specs=pl.BlockSpec(memory_space=pltpu.VMEM),
        scratch_shapes=[
            pltpu.VMEM((NYL, 2 * half, feat), BF16),
            pltpu.VMEM((4, NYL, feat, 2 * seq), BF16),
            pltpu.VMEM((NYL, NZ, seq, width), BF16),
            pltpu.VMEM(basis_in.shape, BF16),
            pltpu.VMEM((seq, width), BF16),
            pltpu.VMEM((4, 2 * seq, 2 * width), BF16),
            pltpu.VMEM((4, NZ, chunk, seq), BF16),
            pltpu.VMEM((4, NZ, chunk, seq), BF16),
            pltpu.VMEM((4, NZ * chunk, seq), BF16),
            pltpu.VMEM((2 * half, 2 * width), F32),
            pltpu.VMEM((half, 2 * width), F32),
            pltpu.VMEM((half, width), BF16),
            pltpu.VMEM((half, width), BF16),
            pltpu.SemaphoreType.DMA((n_sems,)),
            pltpu.SemaphoreType.DMA((n_sems,)),
        ],
        compiler_params=pltpu.CompilerParams(
            collective_id=0, has_side_effects=True, vmem_limit_bytes=48 * 1024 * 1024
        ),
        name="ekfac",
    )(gt, bt, activations[0], basis_in)


def solution(mesh):
    return jax.shard_map(
        shards,
        mesh=mesh,
        in_specs=(P("dp", None, "mp"), P("dp", None, "mp"), P(None, "mp"), P("mp", "dp")),
        out_specs=P("dp", "mp"),
        check_vma=False,
    )
```

```python
import functools

import jax
import jax.numpy as jnp
from jax import lax
from jax.experimental import pallas as pl
from jax.experimental.pallas import tpu as pltpu
from jax.sharding import PartitionSpec as P

MESH = pl.DeviceIdType.MESH
NX, NYH, NYL, NZ = 4, 4, 2, 8
F32, BF16 = jnp.float32, jnp.bfloat16
PAIRS = (((0, 0), (1, 0)), ((2, 0), (0, 1)), ((3, 0), (1, 1)), ((2, 1), (3, 1)))
HOME = {pair[h]: (p, h) for p, pair in enumerate(PAIRS) for h in range(2)}


def kernel(
    dims, bt_ref, gt_hbm, act_hbm, bin_hbm, out_ref,
    bt, gt, g, act, binv, paloc, pa, part, rsb, pg, acc, xrecv, ysend, yrecv,
    send_sems, recv_sems, loc_sems,
):
    feat, seq, half, chunk, width = dims
    dp, mp = lax.axis_index("dp"), lax.axis_index("mp")
    core, x, yh = dp % 2, (dp // 2) % NX, dp // (2 * NX)
    yl, z = mp // NZ, mp % NZ

    def dev(yh_=None, x_=None, c_=None, yl_=None, z_=None):
        yh_ = yh if yh_ is None else yh_
        x_ = x if x_ is None else x_
        c_ = core if c_ is None else c_
        yl_ = yl if yl_ is None else yl_
        z_ = z if z_ is None else z_
        return ((yh_ * NX + x_) * 2 + c_, yl_ * NZ + z_)

    sibling = dev(c_=1 - core)
    ypart = dev(yl_=1 - yl)
    xn = {1: dev(x_=(x + 1) % NX), -1: dev(x_=(x + NX - 1) % NX)}
    zn = {k: dev(z_=(z + NZ + k) % NZ) for k in (1, -1, 2, -2)}

    y = yh * NYL + yl
    ny = NYH * NYL

    def ydev(k):
        yy = (y + ny + k) % ny
        return dev(yh_=yy // NYL, yl_=yy % NYL)

    sigma = 1 - 2 * (yh % 2)
    inner = yl == yh % 2
    outer = yl != yh % 2

    def own_block():
        p, h = HOME[0, 0]
        return g.at[p, 0, :, h * seq:(h + 1) * seq]

    pltpu.make_async_copy(gt_hbm, gt, loc_sems.at[0]).start()
    pltpu.make_async_copy(act_hbm, act.at[0, z], loc_sems.at[1]).start()
    pltpu.make_async_copy(bin_hbm, binv, loc_sems.at[2]).start()
    pl.when(inner)(lambda: pltpu.make_async_copy(gt_hbm, own_block(), loc_sems.at[3]).start())

    barrier = pltpu.get_barrier_semaphore()
    peers = [sibling, xn[1], xn[-1], zn[1], zn[-1], zn[2], zn[-2], ydev(1), ydev(-1), ydev(2), ydev(-2)]
    for peer in peers:
        pl.semaphore_signal(barrier, inc=1, device_id=peer, device_id_type=MESH)
    pl.semaphore_wait(barrier, len(peers))

    counter = [0]
    sent = []

    def take(n=1):
        base = counter[0]
        counter[0] += n
        return base

    def copy_to(src, dst, ssem, rsem, to):
        return pltpu.make_async_remote_copy(
            src_ref=src, dst_ref=dst, send_sem=send_sems.at[ssem], recv_sem=recv_sems.at[rsem],
            device_id=to, device_id_type=MESH,
        )

    def send(src, dst, ssem, rsem, to):
        copy = copy_to(src, dst, ssem, rsem, to)
        copy.start()
        sent.append(copy)

    def send_when(cond, src, dst, ssem, rsem, to):
        copy = copy_to(src, dst, ssem, rsem, to)
        pl.when(cond)(copy.start)
        sent.append((cond, copy))

    def arrived(dst, rsem):
        pltpu.make_async_copy(dst, dst, recv_sems.at[rsem]).wait()

    s_bt = take(6)
    s_act0 = take(1)
    s_gy, s_gx = take(10), take(16)
    s_py, s_px = take(10), take(16)
    s_actz = take(16)
    s_rs, s_ag = take(32), take(32)
    s_out = take(4)

    def y_start(src, src_half, place, base):
        send_when(outer, src, place(0, 0, 1), base, base, ydev(1))
        send_when(outer, src, place(0, 0, 1), base + 1, base, ydev(-1))
        send_when(inner, src, place(0, 0, 0), base, base + 1, ydev(2 * sigma))
        send_when(inner, src_half(0), place(0, 1, 0, 0), base + 1, base + 3, ydev(-2 * sigma))
        send_when(inner, src_half(1), place(0, 1, 0, 1), base + 2, base + 4, ydev(-2 * sigma))

    def x_send(place, xbase, a, f):
        for d, slot in ((1, 1), (-1, 2)):
            s = xbase + slot * 4 + a * 2 + f
            send(place(0, a, f), place(slot, a, f), s, s, xn[d])

    def y_near_other(place, base, xbase):
        arrived(place(0, 0, 1), base)
        send(place(0, 0, 1), place(0, 1, 1), base + 3, base + 2, ydev(-2 * sigma))
        x_send(place, xbase, 0, 1)

    def y_near_own_inner(place, xbase, ready):
        def go():
            ready()
            for d, slot in ((1, 1), (-1, 2)):
                s = xbase + slot * 4
                copy_to(place(0, 0, 0), place(slot, 0, 0), s, s, xn[d]).start()

        pl.when(inner)(go)

    def y_near_own_outer(place, base, xbase):
        def go():
            arrived(place(0, 0, 0), base + 1)
            copy_to(place(0, 0, 0, 0), place(0, 1, 0, 0), base + 4, base + 3, ydev(-2 * sigma)).start()
            for d, slot in ((1, 1), (-1, 2)):
                s = xbase + slot * 4
                copy_to(place(0, 0, 0), place(slot, 0, 0), s, s, xn[d]).start()

        pl.when(outer)(go)
        sent.append((outer, copy_to(place(0, 0, 0, 0), place(0, 1, 0, 0), base + 4, base + 3, ydev(-2 * sigma))))
        for d, slot in ((1, 1), (-1, 2)):
            s = xbase + slot * 4
            sent.append(copy_to(place(0, 0, 0), place(slot, 0, 0), s, s, xn[d]))

    def y_far_other(place, base, xbase):
        arrived(place(0, 1, 1), base + 2)
        x_send(place, xbase, 1, 1)

    def y_far_own(place, base, xbase):
        arrived(place(0, 1, 0, 1), base + 4)
        send_when(outer, place(0, 1, 0, 1), place(0, 1, 0, 1), base + 5, base + 4, ydev(2 * sigma))
        arrived(place(0, 1, 0, 0), base + 3)
        x_send(place, xbase, 1, 0)

    def x_near(place, xbase, a, f):
        for d, slot in ((1, 1), (-1, 2)):
            arrived(place(slot, a, f), xbase + slot * 4 + a * 2 + f)
            if f == slot - 1:
                s = xbase + 12 + a * 2 + f
                send(place(slot, a, f), place(3, a, f), s, s, xn[d])

    def x_far(place, xbase, a, f):
        arrived(place(3, a, f), xbase + 12 + a * 2 + f)

    cut = (feat // 2 + 15) // 16 * 16
    g_parts = {None: slice(None), 0: slice(0, cut), 1: slice(cut, feat)}
    p_parts = {None: (0, seq), 0: (0, seq // 2), 1: (seq // 2, seq)}

    def g_place(slot, a, f, part_=None):
        p, h = HOME[slot, a]
        return g.at[p, f, g_parts[part_], h * seq:(h + 1) * seq]

    def p_place(slot, a, f, part_=None):
        lo, hi = p_parts[part_]
        return pa.at[slot, a * seq + lo:a * seq + hi, f * width:(f + 1) * width]

    def gt_half(i):
        return gt.at[g_parts[i], :]

    def paloc_half(i):
        return paloc.at[slice(*p_parts[i]), :]

    def bt_place(f, c, i):
        return bt.at[f, pl.ds(pl.multiple_of(c * half + i * chunk, 16), chunk), :]

    def bt_src(i):
        return bt_ref.at[i * chunk:(i + 1) * chunk, :]

    def start():
        pltpu.make_async_copy(act_hbm, act.at[0, z], loc_sems.at[1]).wait()
        send(act.at[0, z], act.at[1, z], s_act0, s_act0, ypart)
        pltpu.make_async_copy(gt_hbm, gt, loc_sems.at[0]).wait()
        y_start(gt, gt_half, g_place, s_gy)

    def own_ready():
        pltpu.make_async_copy(gt_hbm, own_block(), loc_sems.at[3]).wait()

    def bt_send(i):
        send(bt_src(i), bt_place(1, core, i), s_bt + 2 + i, s_bt + 2 + i, ypart)
        send(bt_src(i), bt_place(0, core, i), s_bt + i, s_bt + i, sibling)

    def bt_own():
        bt[0, pl.ds(pl.multiple_of(core * half, 16), half), :] = bt_ref[...]

    def bt_forward(i):
        arrived(bt_place(1, core, i), s_bt + 2 + i)
        send(bt_place(1, core, i), bt_place(1, core, i), s_bt + 4 + i, s_bt + 4 + i, sibling)

    def bt_ready():
        for i in range(2):
            arrived(bt_place(0, 1 - core, i), s_bt + i)
            arrived(bt_place(1, 1 - core, i), s_bt + 4 + i)

    def act_send(f, owner, k, tag):
        send(act.at[f, owner], act.at[f, owner], s_actz + tag, s_actz + tag, zn[k])

    def act_tag(f, d, dist):
        return f * 8 + (0 if d == 1 else 4) + dist - 1

    def act_first(f):
        if f == 1:
            arrived(act.at[1, z], s_act0)
        for dist in (2, 1):
            for d in (1, -1):
                act_send(f, z, d * dist, act_tag(f, d, dist))

    def act_wait(f, d, dist):
        arrived(act.at[f, (z + NZ - d * dist) % NZ], s_actz + act_tag(f, d, dist))

    def act_forward():
        for f in range(2):
            for d in (1, -1):
                act_wait(f, d, 2)
                owner = (z + NZ - 2 * d) % NZ
                if (f == 0) == (d == 1):
                    act_send(f, owner, 2 * d, act_tag(f, d, 4))
                act_send(f, owner, d, act_tag(f, d, 3))

    def act_rest():
        for dist in (1, 3, 4):
            for f in range(2):
                for d in (1, -1):
                    if dist < 4 or (f == 0) == (d == 1):
                        act_wait(f, d, dist)

    def project_acts():
        pltpu.make_async_copy(bin_hbm, binv, loc_sems.at[2]).wait()
        total = jnp.zeros((seq, width), F32)
        for f in range(2):
            low = (yl if f == 0 else 1 - yl) * NZ

            def body(i, total, f=f, low=low):
                rows = pl.ds(pl.multiple_of((low + i) * width, 128), width)
                return total + jnp.dot(act[f, i], binv[rows, :], preferred_element_type=F32)

            total = lax.fori_loop(0, NZ, body, total)
        paloc[...] = total.astype(BF16)

        def keep():
            pa[0, :seq, :width] = total.astype(BF16)

        pl.when(inner)(keep)

    def pa_start():
        y_start(paloc, paloc_half, p_place, s_py)

    def project(grp):
        def body(r, carry):
            rows = pl.ds(pl.multiple_of(r * chunk, 16), chunk)
            t = jnp.dot(bt[0, rows, :], g[grp, 0], preferred_element_type=F32)
            t = t + jnp.dot(bt[1, rows, :], g[grp, 1], preferred_element_type=F32)
            t = t.astype(BF16)
            part[grp, r] = t[:, :seq]
            part[grp, r + 4] = t[:, seq:]
            return carry

        lax.fori_loop(0, 4, body, 0)

    def rlen(grp, d):
        return 4 if (grp % 2 == 0) == (d == 1) else 3

    def rs_slot(d, k):
        return (0 if d == 1 else 4) + k

    def rs_step(grp, k):
        for d in (1, -1):
            n = rlen(grp, d)
            if k < n:
                j = (z + NZ + d * (n - k)) % NZ
                if k == 0:
                    src = part.at[grp, j]
                else:
                    slot = rs_slot(d, k - 1)
                    src = rsb.at[grp, slot]
                    arrived(src, s_rs + grp * 8 + slot)
                    rsb[grp, slot] = (rsb[grp, slot].astype(F32) + part[grp, j].astype(F32)).astype(BF16)
                s = s_rs + grp * 8 + rs_slot(d, k)
                send(src, rsb.at[grp, rs_slot(d, k)], s, s, zn[d])

    def pg_place(grp, j):
        return pg.at[grp, pl.ds(pl.multiple_of(j * chunk, 16), chunk), :]

    def ag_sem(grp, d, k):
        return s_ag + grp * 8 + rs_slot(d, k)

    def rs_last(grp):
        total = part[grp, z].astype(F32)
        for d in (1, -1):
            slot = rs_slot(d, rlen(grp, d) - 1)
            arrived(rsb.at[grp, slot], s_rs + grp * 8 + slot)
            total = total + rsb[grp, slot].astype(F32)
        pg[grp, pl.ds(pl.multiple_of(z * chunk, 16), chunk), :] = total.astype(BF16)
        for d in (1, -1):
            send(pg_place(grp, z), pg_place(grp, z), ag_sem(grp, d, 0), ag_sem(grp, d, 0), zn[d])

    def ag_step(grp, k):
        for d in (1, -1):
            n = rlen(grp, d)
            if k <= n:
                j = (z + NZ - d * k) % NZ
                arrived(pg_place(grp, j), ag_sem(grp, d, k - 1))
                if k < n:
                    send(pg_place(grp, j), pg_place(grp, j), ag_sem(grp, d, k), ag_sem(grp, d, k), zn[d])

    def squares(grp, lo, hi):
        def body(r, carry):
            rows = pl.ds(pl.multiple_of(r * chunk, 16), chunk)
            total = None if grp == 0 else acc[rows, lo:hi]
            for a in range(2):
                lhs = pg[grp, pl.ds(pl.multiple_of((a * 4 + r) * chunk, 16), chunk), :]
                slot, far = PAIRS[grp][a]
                t = jnp.dot(lhs, pa[slot, far * seq:(far + 1) * seq, lo:hi], preferred_element_type=F32)
                total = t * t if total is None else total + t * t
            acc[rows, lo:hi] = total
            return carry

        lax.fori_loop(0, 4, body, 0)

    mine = pl.ds(pl.multiple_of(core * half, 8), half)
    theirs = pl.ds(pl.multiple_of((1 - core) * half, 8), half)
    spans = (slice(0, width), slice(width, 2 * width))

    def out_core(i):
        send(acc.at[theirs, spans[i]], xrecv.at[:, spans[i]], s_out + i, s_out + i, sibling)

    def out_y():
        arrived(xrecv.at[:, spans[1]], s_out + 1)
        for i in range(2):
            rows = slice(i * chunk, (i + 1) * chunk)
            ysend[rows, :] = (acc[pl.ds(pl.multiple_of(core * half + i * chunk, 8), chunk), spans[1]]
                              + xrecv[rows, spans[1]]).astype(BF16)
            send(ysend.at[rows, :], yrecv.at[rows, :], s_out + 2 + i, s_out + 2 + i, ypart)

    def out_last():
        arrived(xrecv.at[:, spans[0]], s_out)
        total = out_ref.shape[0]
        for i in range(2):
            lo, hi = i * chunk, min((i + 1) * chunk, total)
            arrived(yrecv.at[lo:(i + 1) * chunk, :], s_out + 2 + i)
            own = acc[pl.ds(pl.multiple_of(core * half + lo, 8), hi - lo), spans[0]] + xrecv[lo:hi, spans[0]]
            out_ref[lo:hi, :] = (own + yrecv[lo:hi, :].astype(F32)) * (1.0 / 4096.0)

    steps = []

    def at(t, fn, *args):
        steps.append((t, len(steps), functools.partial(fn, *args)))

    at(0, start)
    at(0.05, act_first, 0)
    at(0.1, y_near_own_inner, g_place, s_gx, own_ready)
    at(0.2, bt_send, 0)
    at(0.3, bt_own)
    at(4, act_first, 1)
    at(6.5, y_near_other, g_place, s_gy, s_gx)
    at(6.6, bt_send, 1)
    at(9, y_near_own_outer, g_place, s_gy, s_gx)
    at(13, x_near, g_place, s_gx, 0, 0)
    at(13.1, x_near, g_place, s_gx, 0, 1)
    at(14, bt_forward, 0)
    at(16.5, act_forward)
    at(17, y_far_other, g_place, s_gy, s_gx)
    at(20, y_far_own, g_place, s_gy, s_gx)
    at(22, bt_forward, 1)
    at(24, bt_ready)
    at(24.1, project, 0)
    at(24.1, rs_step, 0, 0)
    at(24.2, project, 1)
    at(24.2, rs_step, 1, 0)
    at(25.1, x_near, g_place, s_gx, 1, 1)
    at(25.2, act_rest)
    at(25.3, project_acts)
    at(25.4, pa_start)
    at(27, x_near, g_place, s_gx, 1, 0)
    at(27.9, x_far, g_place, s_gx, 0, 0)
    at(27.9, x_far, g_place, s_gx, 0, 1)
    at(28, project, 2)
    at(28, rs_step, 2, 0)
    at(32, x_far, g_place, s_gx, 1, 0)
    at(32, x_far, g_place, s_gx, 1, 1)
    at(32, project, 3)
    at(32, rs_step, 3, 0)
    at(31, y_near_own_inner, p_place, s_px, lambda: None)
    at(31.1, y_near_other, p_place, s_py, s_px)
    at(31.2, y_near_own_outer, p_place, s_py, s_px)
    at(36, y_far_other, p_place, s_py, s_px)
    at(36.1, y_far_own, p_place, s_py, s_px)
    for i, (a, f) in enumerate(((0, 0), (0, 1), (1, 1), (1, 0))):
        at(41 + 0.1 * i, x_near, p_place, s_px, a, f)
        at(46.5, x_far, p_place, s_px, a, f)
    for grp, r0, a0 in ((0, 27.5, 38), (1, 27.8, 38.3), (2, 31.8, 42.3), (3, 36, 46.5)):
        for k in (1, 2, 3):
            at(r0 + 3.5 * (k - 1), rs_step, grp, k)
        at(a0, rs_last, grp)
        for k in (1, 2, 3, 4):
            at(a0 + 3.5 * k, ag_step, grp, k)
    at(53, squares, 0, 0, 2 * width)
    at(54, squares, 1, 0, 2 * width)
    at(57.1, squares, 2, 0, 2 * width)
    at(62, squares, 3, width, 2 * width)
    at(62.1, out_core, 1)
    at(62.2, squares, 3, 0, width)
    at(62.3, out_core, 0)
    at(63, out_y)
    at(64, out_last)
    for _, _, fn in sorted(steps, key=lambda s: (s[0], s[1])):
        fn()
    for item in sent:
        if isinstance(item, tuple):
            pl.when(item[0])(item[1].wait_send)
        else:
            item.wait_send()


def shards(activations, gradients, basis_in, basis_out):
    seq, feat = gradients.shape[1:]
    cols = basis_out.shape[1]
    width = basis_in.shape[1]
    half = (cols + 31) // 32 * 32
    chunk = half // 2
    gt = gradients[0].T
    bt = jnp.pad(basis_out.T, ((0, half - cols), (0, 0)))
    dims = (feat, seq, half, chunk, width)
    n_sems = 184
    return pl.pallas_call(
        functools.partial(kernel, dims),
        out_shape=jax.ShapeDtypeStruct((cols, width), F32),
        in_specs=[pl.BlockSpec(memory_space=pltpu.VMEM)] + [pl.BlockSpec(memory_space=pltpu.HBM)] * 3,
        out_specs=pl.BlockSpec(memory_space=pltpu.VMEM),
        scratch_shapes=[
            pltpu.VMEM((NYL, 2 * half, feat), BF16),
            pltpu.VMEM((feat, seq), BF16),
            pltpu.VMEM((4, NYL, feat, 2 * seq), BF16),
            pltpu.VMEM((NYL, NZ, seq, width), BF16),
            pltpu.VMEM(basis_in.shape, BF16),
            pltpu.VMEM((seq, width), BF16),
            pltpu.VMEM((4, 2 * seq, 2 * width), BF16),
            pltpu.VMEM((4, NZ, chunk, seq), BF16),
            pltpu.VMEM((4, NZ, chunk, seq), BF16),
            pltpu.VMEM((4, NZ * chunk, seq), BF16),
            pltpu.VMEM((2 * half, 2 * width), F32),
            pltpu.VMEM((half, 2 * width), F32),
            pltpu.VMEM((half, width), BF16),
            pltpu.VMEM((half, width), BF16),
            pltpu.SemaphoreType.DMA((n_sems,)),
            pltpu.SemaphoreType.DMA((n_sems,)),
            pltpu.SemaphoreType.DMA((4,)),
        ],
        compiler_params=pltpu.CompilerParams(
            collective_id=0, has_side_effects=True, vmem_limit_bytes=60 * 1024 * 1024
        ),
        name="ekfac",
    )(bt, gt, activations[0], basis_in)


def solution(mesh):
    return jax.shard_map(
        shards,
        mesh=mesh,
        in_specs=(P("dp", None, "mp"), P("dp", None, "mp"), P(None, "mp"), P("mp", "dp")),
        out_specs=P("dp", "mp"),
        check_vma=False,
    )
```

```python
import functools

import jax
import jax.numpy as jnp
from jax import lax
from jax.experimental import pallas as pl
from jax.experimental.pallas import tpu as pltpu
from jax.sharding import PartitionSpec as P

MESH = pl.DeviceIdType.MESH
NX, NYH, NYL, NZ = 4, 4, 2, 8
F32, BF16 = jnp.float32, jnp.bfloat16
SETS = (((0, 0), (1, 0), (2, 0), (0, 1)), ((3, 0), (1, 1), (2, 1), (3, 1)))
HOME = {key: (k, pos) for k, keys in enumerate(SETS) for pos, key in enumerate(keys)}


def kernel(
    dims, basis_hbm, gt_hbm, act_hbm, bin_hbm, out_ref,
    raw, bt, gt, g, act, binv, paloc, pa, part, rsb, pg, acc, xrecv, ysend, yrecv,
    send_sems, recv_sems, loc_sems,
):
    feat, seq, half, chunk, width = dims
    dp, mp = lax.axis_index("dp"), lax.axis_index("mp")
    core, x, yh = dp % 2, (dp // 2) % NX, dp // (2 * NX)
    yl, z = mp // NZ, mp % NZ

    def dev(yh_=None, x_=None, c_=None, yl_=None, z_=None):
        yh_ = yh if yh_ is None else yh_
        x_ = x if x_ is None else x_
        c_ = core if c_ is None else c_
        yl_ = yl if yl_ is None else yl_
        z_ = z if z_ is None else z_
        return ((yh_ * NX + x_) * 2 + c_, yl_ * NZ + z_)

    sibling = dev(c_=1 - core)
    ypart = dev(yl_=1 - yl)
    xn = {1: dev(x_=(x + 1) % NX), -1: dev(x_=(x + NX - 1) % NX)}
    zn = {k: dev(z_=(z + NZ + k) % NZ) for k in (1, -1, 2, -2)}

    y = yh * NYL + yl
    ny = NYH * NYL

    def ydev(k):
        yy = (y + ny + k) % ny
        return dev(yh_=yy // NYL, yl_=yy % NYL)

    sigma = 1 - 2 * (yh % 2)
    inner = yl == yh % 2
    outer = yl != yh % 2

    def own_block():
        return g.at[0, 0, :, :seq]

    pltpu.make_async_copy(gt_hbm, gt, loc_sems.at[0]).start()
    pltpu.make_async_copy(act_hbm, act.at[0, z], loc_sems.at[1]).start()
    pltpu.make_async_copy(basis_hbm, raw, loc_sems.at[4]).start()
    pltpu.make_async_copy(bin_hbm, binv, loc_sems.at[2]).start()
    pl.when(inner)(lambda: pltpu.make_async_copy(gt_hbm, own_block(), loc_sems.at[3]).start())

    barrier = pltpu.get_barrier_semaphore()
    peers = [sibling, xn[1], xn[-1], zn[1], zn[-1], zn[2], zn[-2], ydev(1), ydev(-1), ydev(2), ydev(-2)]
    for peer in peers:
        pl.semaphore_signal(barrier, inc=1, device_id=peer, device_id_type=MESH)
    pl.semaphore_wait(barrier, len(peers))

    refs = (basis_hbm, gt_hbm, act_hbm, bin_hbm, out_ref, raw, bt, gt, g, act, binv, paloc, pa, part, rsb, pg, acc,
            xrecv, ysend, yrecv, send_sems, recv_sems, loc_sems)
    where = (core, yl, z, sigma, sibling, ypart, xn, zn, ydev, own_block)
    pl.when(inner)(lambda: program(True, dims, where, *refs))
    pl.when(outer)(lambda: program(False, dims, where, *refs))


def program(
    is_inner, dims, where, basis_hbm, gt_hbm, act_hbm, bin_hbm, out_ref, raw, bt, gt, g, act, binv, paloc, pa, part,
    rsb, pg, acc, xrecv, ysend, yrecv, send_sems, recv_sems, loc_sems,
):
    feat, seq, half, chunk, width = dims
    core, yl, z, sigma, sibling, ypart, xn, zn, ydev, own_block = where
    counter = [0]

    def take(n=1):
        base = counter[0]
        counter[0] += n
        return base

    S_GY, S_GX, S_PY, S_PX, S_ACT, S_BT, S_RS, S_AG, S_OC, S_OY = range(10)

    def send(src, dst, kind, rsem, to):
        pltpu.make_async_remote_copy(
            src_ref=src, dst_ref=dst, send_sem=send_sems.at[kind], recv_sem=recv_sems.at[rsem],
            device_id=to, device_id_type=MESH,
        ).start()

    def arrived(dst, rsem):
        pltpu.make_async_copy(dst, dst, recv_sems.at[rsem]).wait()

    s_bt = take(6)
    s_act0 = take(1)
    s_gy, s_gx = take(8), take(24)
    s_py, s_px = take(8), take(12)
    s_actz = take(16)
    s_rs, s_ag = take(32), take(32)
    s_out = take(6)

    def num(part):
        return 1 if part == 1 else 0

    def y_start(pat):
        place, source, parts, base, _, kind, _ = pat

        def from_outer():
            for p in parts:
                for d in (1, -1):
                    send(source(p), place(0, 0, 1, p), kind, base + num(p), ydev(d))

        def from_inner():
            for p in parts:
                send(source(p), place(0, 0, 0, p), kind, base + 2 + num(p), ydev(2 * sigma))
                for h in (0, 1) if p is None else (p,):
                    send(source(h), place(0, 1, 0, h), kind, base + 6 + h, ydev(-2 * sigma))

        from_inner() if is_inner else from_outer()

    def x_send(pat, a, f, p):
        place, _, parts, _, base, _, kind = pat
        for d, slot in ((1, 1), (-1, 2)):
            s = base + ((slot - 1) * 4 + a * 2 + f) * len(parts) + num(p)
            send(place(0, a, f, p), place(slot, a, f, p), kind, s, xn[d])

    def y_near_other(pat, p):
        place, _, _, base, _, kind, _ = pat
        arrived(place(0, 0, 1, p), base + num(p))
        send(place(0, 0, 1, p), place(0, 1, 1, p), kind, base + 4 + num(p), ydev(-2 * sigma))
        x_send(pat, 0, 1, p)

    def y_near_own(pat):
        place, _, parts, base, _, kind, _ = pat
        for p in parts:
            if not is_inner:
                arrived(place(0, 0, 0, p), base + 2 + num(p))
                if p != 1:
                    send(place(0, 0, 0, 0), place(0, 1, 0, 0), kind, base + 6, ydev(-2 * sigma))
            x_send(pat, 0, 0, p)

    def y_far_own(pat):
        place, _, parts, base, _, kind, _ = pat
        for h in (1, 0):
            arrived(place(0, 1, 0, h), base + 6 + h)
            if not is_inner and h == 1:
                send(place(0, 1, 0, 1), place(0, 1, 0, 1), kind, base + 7, ydev(2 * sigma))
            if h in parts:
                x_send(pat, 1, 0, h)
        if None in parts:
            x_send(pat, 1, 0, None)

    def y_far_other(pat, p):
        place, _, _, base, _, _, _ = pat
        arrived(place(0, 1, 1, p), base + 4 + num(p))
        x_send(pat, 1, 1, p)

    def x_near(pat, a, f):
        place, _, parts, _, base, _, kind = pat
        for p in parts:
            for d, slot in ((1, 1), (-1, 2)):
                s = base + ((slot - 1) * 4 + a * 2 + f) * len(parts) + num(p)
                arrived(place(slot, a, f, p), s)
                if f == slot - 1:
                    s = base + (8 + a * 2 + f) * len(parts) + num(p)
                    send(place(slot, a, f, p), place(3, a, f, p), kind, s, xn[d])

    def x_far(pat, a, f):
        place, _, parts, _, base, _, _ = pat
        for p in parts:
            arrived(place(3, a, f, p), base + (8 + a * 2 + f) * len(parts) + num(p))

    cut = (feat // 2 + 15) // 16 * 16
    g_parts = {None: slice(None), 0: slice(0, cut), 1: slice(cut, feat)}
    p_parts = {None: (0, seq), 0: (0, seq // 2), 1: (seq // 2, seq)}

    def g_place(slot, a, f, part_=None):
        k, pos = HOME[slot, a]
        return g.at[k, f, g_parts[part_], pos * seq:(pos + 1) * seq]

    def p_place(slot, a, f, part_=None):
        lo, hi = p_parts[part_]
        return pa.at[slot, a * seq + lo:a * seq + hi, f * width:(f + 1) * width]

    def g_source(p):
        return gt.at[g_parts[p], :]

    def p_source(p):
        return paloc.at[slice(*p_parts[p]), :]

    gpat = (g_place, g_source, (0, 1), s_gy, s_gx, S_GY, S_GX)
    ppat = (p_place, p_source, (None,), s_py, s_px, S_PY, S_PX)

    def bt_place(f, c, i):
        return bt.at[f, pl.ds(pl.multiple_of(c * half + i * chunk, 16), chunk), :]

    def start():
        pltpu.make_async_copy(gt_hbm, gt, loc_sems.at[0]).wait()
        y_start(gpat)
        pltpu.make_async_copy(act_hbm, act.at[0, z], loc_sems.at[1]).wait()
        send(act.at[0, z], act.at[1, z], S_ACT, s_act0, ypart)

    def g_own():
        if is_inner:
            pltpu.make_async_copy(gt_hbm, own_block(), loc_sems.at[3]).wait()
        y_near_own(gpat)

    def bt_own():
        pltpu.make_async_copy(basis_hbm, raw, loc_sems.at[4]).wait()
        turned = raw[...].T
        bt[0, pl.ds(pl.multiple_of(core * half, 16), turned.shape[0]), :] = turned

    def bt_rows(f, lo, hi):
        return bt.at[f, pl.ds(pl.multiple_of(core * half + lo, 16), hi - lo), :]

    def bt_send(i, pieces=(0, 1)):
        split = chunk // 32 * 16
        for lo, hi in [((0, split), (split, chunk))[piece] for piece in pieces]:
            lo, hi = i * chunk + lo, i * chunk + hi
            send(bt_rows(0, lo, hi), bt_rows(1, lo, hi), S_BT, s_bt + 2 + i, ypart)
            send(bt_rows(0, lo, hi), bt_rows(0, lo, hi), S_BT, s_bt + i, sibling)

    def bt_forward(i):
        arrived(bt_place(1, core, i), s_bt + 2 + i)
        send(bt_place(1, core, i), bt_place(1, core, i), S_BT, s_bt + 4 + i, sibling)

    def bt_ready(i):
        arrived(bt_place(0, 1 - core, i), s_bt + i)
        arrived(bt_place(1, 1 - core, i), s_bt + 4 + i)

    def act_send(f, owner, k, tag):
        send(act.at[f, owner], act.at[f, owner], S_ACT, s_actz + tag, zn[k])

    def act_tag(f, d, dist):
        return f * 8 + (0 if d == 1 else 4) + dist - 1

    def act_first(f):
        if f == 1:
            arrived(act.at[1, z], s_act0)
        for dist in (2, 1):
            for d in (1, -1):
                act_send(f, z, d * dist, act_tag(f, d, dist))

    def act_wait(f, d, dist):
        arrived(act.at[f, (z + NZ - d * dist) % NZ], s_actz + act_tag(f, d, dist))

    def act_forward():
        for f in range(2):
            for d in (1, -1):
                act_wait(f, d, 2)
                owner = (z + NZ - 2 * d) % NZ
                if (f == 0) == (d == 1):
                    act_send(f, owner, 2 * d, act_tag(f, d, 4))
                act_send(f, owner, d, act_tag(f, d, 3))

    def act_rest():
        for dist in (1, 3, 4):
            for f in range(2):
                for d in (1, -1):
                    if dist < 4 or (f == 0) == (d == 1):
                        act_wait(f, d, dist)

    def project_acts():
        pltpu.make_async_copy(bin_hbm, binv, loc_sems.at[2]).wait()
        total = jnp.zeros((seq, width), F32)
        for f in range(2):
            low = (yl if f == 0 else 1 - yl) * NZ

            def body(i, total, f=f, low=low):
                rows = pl.ds(pl.multiple_of((low + i) * width, 128), width)
                return total + jnp.dot(act[f, i], binv[rows, :], preferred_element_type=F32)

            total = lax.fori_loop(0, NZ, body, total)
        paloc[...] = total.astype(BF16)

        if is_inner:
            pa[0, :seq, :width] = total.astype(BF16)

    def pa_start():
        y_start(ppat)

    def project(grp):
        a, i = grp // 2, grp % 2

        def body(c, carry):
            rows = pl.ds(pl.multiple_of(c * half + i * chunk, 16), chunk)
            for pair in range(2):
                cols = slice(2 * pair * seq, 2 * (pair + 1) * seq)
                t = jnp.dot(bt[0, rows, :], g[a, 0, :, cols], preferred_element_type=F32)
                t = t + jnp.dot(bt[1, rows, :], g[a, 1, :, cols], preferred_element_type=F32)
                t = t.astype(BF16)
                part[grp, c * 4 + 2 * pair] = t[:, :seq]
                part[grp, c * 4 + 2 * pair + 1] = t[:, seq:]
            return carry

        lax.fori_loop(0, 2, body, 0)

    def rlen(grp, d):
        return 4 if (grp % 2 == 0) == (d == 1) else 3

    def rs_slot(d, k):
        return (0 if d == 1 else 4) + k

    def rs_step(grp, k):
        for d in (1, -1):
            n = rlen(grp, d)
            if k < n:
                j = (z + NZ + d * (n - k)) % NZ
                if k == 0:
                    src = part.at[grp, j]
                else:
                    slot = rs_slot(d, k - 1)
                    src = rsb.at[grp, slot]
                    arrived(src, s_rs + grp * 8 + slot)
                    rsb[grp, slot] = (rsb[grp, slot].astype(F32) + part[grp, j].astype(F32)).astype(BF16)
                s = s_rs + grp * 8 + rs_slot(d, k)
                send(src, rsb.at[grp, rs_slot(d, k)], S_RS, s, zn[d])

    def pg_place(grp, j):
        return pg.at[grp, pl.ds(pl.multiple_of(j * chunk, 16), chunk), :]

    def ag_sem(grp, d, k):
        return s_ag + grp * 8 + rs_slot(d, k)

    def rs_last(grp):
        total = part[grp, z].astype(F32)
        for d in (1, -1):
            slot = rs_slot(d, rlen(grp, d) - 1)
            arrived(rsb.at[grp, slot], s_rs + grp * 8 + slot)
            total = total + rsb[grp, slot].astype(F32)
        pg[grp, pl.ds(pl.multiple_of(z * chunk, 16), chunk), :] = total.astype(BF16)
        for d in (1, -1):
            send(pg_place(grp, z), pg_place(grp, z), S_AG, ag_sem(grp, d, 0), zn[d])

    def ag_step(grp, k):
        for d in (1, -1):
            n = rlen(grp, d)
            if k <= n:
                j = (z + NZ - d * k) % NZ
                arrived(pg_place(grp, j), ag_sem(grp, d, k - 1))
                if k < n:
                    send(pg_place(grp, j), pg_place(grp, j), S_AG, ag_sem(grp, d, k), zn[d])

    def squares(grp, lo, hi):
        a, i = grp // 2, grp % 2

        def body(c, carry):
            rows = pl.ds(pl.multiple_of(c * half + i * chunk, 16), chunk)
            total = None if a == 0 else acc[rows, lo:hi]
            for pos, (slot, far) in enumerate(SETS[a]):
                lhs = pg[grp, pl.ds(pl.multiple_of((c * 4 + pos) * chunk, 16), chunk), :]
                t = jnp.dot(lhs, pa[slot, far * seq:(far + 1) * seq, lo:hi], preferred_element_type=F32)
                total = t * t if total is None else total + t * t
            acc[rows, lo:hi] = total
            return carry

        lax.fori_loop(0, 2, body, 0)

    spans = (slice(0, width), slice(width, 2 * width))

    def acc_rows(c, i):
        return pl.ds(pl.multiple_of(c * half + i * chunk, 8), chunk)

    def out_core(i, f):
        dst = xrecv.at[i * chunk:(i + 1) * chunk, spans[f]]
        send(acc.at[acc_rows(1 - core, i), spans[f]], dst, S_OC, s_out + 2 * i + f, sibling)

    def out_y(i):
        rows = slice(i * chunk, (i + 1) * chunk)
        arrived(xrecv.at[rows, spans[1]], s_out + 2 * i + 1)
        ysend[rows, :] = (acc[acc_rows(core, i), spans[1]] + xrecv[rows, spans[1]]).astype(BF16)
        send(ysend.at[rows, :], yrecv.at[rows, :], S_OY, s_out + 4 + i, ypart)

    def out_last(i):
        rows = slice(i * chunk, (i + 1) * chunk)
        n = min(chunk, out_ref.shape[0] - i * chunk)
        arrived(xrecv.at[rows, spans[0]], s_out + 2 * i)
        own = acc[acc_rows(core, i), spans[0]] + xrecv[rows, spans[0]]
        arrived(yrecv.at[rows, :], s_out + 4 + i)
        own = (own + yrecv[rows, :].astype(F32)) * (1.0 / 4096.0)
        out_ref[i * chunk:i * chunk + n, :] = own[:n]

    steps = []

    def at(t_inner, t_outer, fn, *args):
        steps.append((t_inner if is_inner else t_outer, len(steps), functools.partial(fn, *args)))

    at(0, 0, start)
    at(0.04, 11, g_own)
    at(0.05, 0.05, act_first, 0)
    at(0.3, 0.3, bt_own)
    at(0.35, 6.4, bt_send, 0, (0,))
    at(0.35, 11.2, bt_send, 0, (1,))
    at(0.36, 11.25, bt_send, 1)
    at(4, 4.5, y_near_other, gpat, 0)
    at(5.8, 6.3, y_near_other, gpat, 1)
    at(6.5, 15.5, x_near, gpat, 0, 0)
    at(15.45, 11.1, y_far_own, gpat)
    at(10.5, 12, x_near, gpat, 0, 1)
    at(11, 13, y_far_other, gpat, 0)
    at(12.5, 14.5, y_far_other, gpat, 1)
    at(12.6, 12.1, act_first, 1)
    at(15.3, 17, act_forward)
    at(15.5, 18.2, bt_forward, 0)
    at(28, 22.42, x_far, gpat, 0, 0)
    at(28, 22.42, x_far, gpat, 0, 1)
    at(15.4, 20.5, x_near, gpat, 1, 1)
    at(20.9, 18.5, x_near, gpat, 1, 0)
    at(18.5, 18.6, bt_ready, 0)
    at(18.6, 18.6, project, 0)
    at(18.6, 18.6, rs_step, 0, 0)
    at(21, 19, act_rest)
    at(21, 19, project_acts)
    at(21, 19, pa_start)
    at(22, 22.2, bt_forward, 1)
    at(25, 22.4, bt_ready, 1)
    at(25, 22.4, project, 1)
    at(25, 22.4, rs_step, 1, 0)
    at(28, 28, x_far, gpat, 1, 0)
    at(28, 28, x_far, gpat, 1, 1)
    for grp in (2, 3):
        at(28, 28, project, grp)
        at(28, 28, rs_step, grp, 0)
    at(22, 28.62, y_near_own, ppat)
    at(32.5, 28.61, y_near_other, ppat, None)
    at(41.1, 28.63, y_far_own, ppat)
    at(41, 41, y_far_other, ppat, None)
    for i, (a, f) in enumerate(((0, 0), (0, 1), (1, 1), (1, 0))):
        t = (43, 43, 47.4, 47.4)[i]
        at(t, t, x_near, ppat, a, f)
        t = (48, 48, 54.8, 54.8)[i]
        at(t, t, x_far, ppat, a, f)
    for grp, r0, a0 in ((0, 23, 34), (1, 29, 40.2), (2, 32, 43.3), (3, 32.1, 43.4)):
        for k in (1, 2, 3):
            t = r0 + 3.7 * (k - 1) + (2 if grp == 0 and k > 1 and not is_inner else 0)
            at(t, t, rs_step, grp, k)
        at(a0, a0, rs_last, grp)
        for k in (1, 2, 3, 4):
            t = a0 + 3.7 * k
            at(t, t, ag_step, grp, k)
    at(50, 50, squares, 0, 0, 2 * width)
    at(56, 56, squares, 1, 0, 2 * width)
    at(58.15, 58.15, squares, 2, 0, 2 * width)
    at(58.15, 58.15, out_core, 0, 1)
    at(58.15, 58.15, out_core, 0, 0)
    at(59, 59, squares, 3, width, 2 * width)
    at(59, 59, out_core, 1, 1)
    at(59.1, 59.1, squares, 3, 0, width)
    at(59.2, 59.2, out_core, 1, 0)
    at(59.3, 59.3, out_y, 0)
    at(61, 61, out_y, 1)
    at(62, 62, out_last, 0)
    at(63, 63, out_last, 1)

    def drain():
        def sent(ref, kind):
            pltpu.make_async_copy(ref, ref, send_sems.at[kind]).wait()

        blocks = 3 if is_inner else 4
        sent(g.at[0, 0, :, :blocks * seq], S_GY)
        sent(act.at[0, :blocks], S_PY)
        sent(g.at[:, :, :, seq:], S_GX)
        sent(pa.at[1:], S_PX)
        sent(binv.at[:15 * seq, :], S_ACT)
        sent(bt.at[:, :3 * chunk, :], S_BT)
        sent(rsb.at[:, :7], S_RS)
        sent(rsb.at[:, :7], S_AG)
        sent(xrecv, S_OC)
        sent(yrecv, S_OY)

    at(999, 999, drain)
    assert counter[0] == recv_sems.shape[0]
    for _, _, fn in sorted(steps, key=lambda s: (s[0], s[1])):
        fn()


def shards(activations, gradients, basis_in, basis_out):
    seq, feat = gradients.shape[1:]
    cols = basis_out.shape[1]
    width = basis_in.shape[1]
    half = (cols + 31) // 32 * 32
    chunk = half // 2
    gt = gradients[0].T
    dims = (feat, seq, half, chunk, width)
    return pl.pallas_call(
        functools.partial(kernel, dims),
        out_shape=jax.ShapeDtypeStruct((cols, width), F32),
        in_specs=[pl.BlockSpec(memory_space=pltpu.HBM)] * 4,
        out_specs=pl.BlockSpec(memory_space=pltpu.VMEM),
        scratch_shapes=[
            pltpu.VMEM((feat, cols), BF16),
            pltpu.VMEM((NYL, 2 * half, feat), BF16),
            pltpu.VMEM((feat, seq), BF16),
            pltpu.VMEM((2, NYL, feat, 4 * seq), BF16),
            pltpu.VMEM((NYL, NZ, seq, width), BF16),
            pltpu.VMEM(basis_in.shape, BF16),
            pltpu.VMEM((seq, width), BF16),
            pltpu.VMEM((4, 2 * seq, 2 * width), BF16),
            pltpu.VMEM((4, NZ, chunk, seq), BF16),
            pltpu.VMEM((4, NZ, chunk, seq), BF16),
            pltpu.VMEM((4, NZ * chunk, seq), BF16),
            pltpu.VMEM((2 * half, 2 * width), F32),
            pltpu.VMEM((half, 2 * width), F32),
            pltpu.VMEM((half, width), BF16),
            pltpu.VMEM((half, width), BF16),
            pltpu.SemaphoreType.DMA((10,)),
            pltpu.SemaphoreType.DMA((145,)),
            pltpu.SemaphoreType.DMA((5,)),
        ],
        compiler_params=pltpu.CompilerParams(
            collective_id=0, has_side_effects=True, vmem_limit_bytes=60 * 1024 * 1024
        ),
        name="ekfac",
    )(basis_out, gt, activations[0], basis_in)


def solution(mesh):
    return jax.shard_map(
        shards,
        mesh=mesh,
        in_specs=(P("dp", None, "mp"), P("dp", None, "mp"), P(None, "mp"), P("mp", "dp")),
        out_specs=P("dp", "mp"),
        check_vma=False,
    )
```

```python
import functools

import jax
import jax.numpy as jnp
from jax import lax
from jax.experimental import pallas as pl
from jax.experimental.pallas import tpu as pltpu
from jax.sharding import PartitionSpec as P

MESH = pl.DeviceIdType.MESH
NX, NYH, NYL, NZ = 4, 4, 2, 8
F32, BF16 = jnp.float32, jnp.bfloat16
SETS = (((0, 0), (1, 0), (2, 0), (0, 1)), ((3, 0), (1, 1), (2, 1), (3, 1)))
HOME = {key: (k, pos) for k, keys in enumerate(SETS) for pos, key in enumerate(keys)}


def kernel(
    dims, basis_hbm, gt_hbm, act_hbm, bin_hbm, out_ref,
    raw, bt, gt, g, act, binv, paloc, pa, part, rsb, pg, acc, xrecv, ysend, yrecv,
    send_sems, recv_sems, loc_sems,
):
    feat, seq, half, chunk, width = dims
    dp, mp = lax.axis_index("dp"), lax.axis_index("mp")
    core, x, yh = dp % 2, (dp // 2) % NX, dp // (2 * NX)
    yl, z = mp // NZ, mp % NZ

    def dev(yh_=None, x_=None, c_=None, yl_=None, z_=None):
        yh_ = yh if yh_ is None else yh_
        x_ = x if x_ is None else x_
        c_ = core if c_ is None else c_
        yl_ = yl if yl_ is None else yl_
        z_ = z if z_ is None else z_
        return ((yh_ * NX + x_) * 2 + c_, yl_ * NZ + z_)

    sibling = dev(c_=1 - core)
    ypart = dev(yl_=1 - yl)
    xn = {1: dev(x_=(x + 1) % NX), -1: dev(x_=(x + NX - 1) % NX)}
    zn = {k: dev(z_=(z + NZ + k) % NZ) for k in (1, -1, 2, -2)}

    y = yh * NYL + yl
    ny = NYH * NYL

    def ydev(k):
        yy = (y + ny + k) % ny
        return dev(yh_=yy // NYL, yl_=yy % NYL)

    sigma = 1 - 2 * (yh % 2)
    inner = yl == yh % 2
    outer = yl != yh % 2

    def own_block():
        return g.at[0, 0, :, :seq]

    pltpu.make_async_copy(gt_hbm, gt, loc_sems.at[0]).start()
    pltpu.make_async_copy(act_hbm, act.at[0, z], loc_sems.at[1]).start()
    pltpu.make_async_copy(basis_hbm, raw, loc_sems.at[4]).start()
    pltpu.make_async_copy(bin_hbm, binv, loc_sems.at[2]).start()
    pl.when(inner)(lambda: pltpu.make_async_copy(gt_hbm, own_block(), loc_sems.at[3]).start())

    barrier = pltpu.get_barrier_semaphore()
    peers = [sibling, xn[1], xn[-1], zn[1], zn[-1], zn[2], zn[-2], ydev(1), ydev(-1), ydev(2), ydev(-2)]
    for peer in peers:
        pl.semaphore_signal(barrier, inc=1, device_id=peer, device_id_type=MESH)
    pl.semaphore_wait(barrier, len(peers))

    refs = (basis_hbm, gt_hbm, act_hbm, bin_hbm, out_ref, raw, bt, gt, g, act, binv, paloc, pa, part, rsb, pg, acc,
            xrecv, ysend, yrecv, send_sems, recv_sems, loc_sems)
    where = (core, yl, z, sigma, sibling, ypart, xn, zn, ydev, own_block)
    pl.when(inner)(lambda: program(True, dims, where, *refs))
    pl.when(outer)(lambda: program(False, dims, where, *refs))


def program(
    is_inner, dims, where, basis_hbm, gt_hbm, act_hbm, bin_hbm, out_ref, raw, bt, gt, g, act, binv, paloc, pa, part,
    rsb, pg, acc, xrecv, ysend, yrecv, send_sems, recv_sems, loc_sems,
):
    feat, seq, half, chunk, width = dims
    core, yl, z, sigma, sibling, ypart, xn, zn, ydev, own_block = where
    counter = [0]

    def take(n=1):
        base = counter[0]
        counter[0] += n
        return base

    S_GY, S_GX, S_PY, S_PX, S_ACT, S_BT, S_RS, S_AG, S_OC, S_OY = range(10)

    def send(src, dst, kind, rsem, to):
        pltpu.make_async_remote_copy(
            src_ref=src, dst_ref=dst, send_sem=send_sems.at[kind], recv_sem=recv_sems.at[rsem],
            device_id=to, device_id_type=MESH,
        ).start()

    def arrived(dst, rsem):
        pltpu.make_async_copy(dst, dst, recv_sems.at[rsem]).wait()

    s_bt = take(6)
    s_act0 = take(1)
    s_gy, s_gx = take(8), take(24)
    s_py, s_px = take(8), take(12)
    s_actz = take(16)
    s_rs, s_ag = take(32), take(32)
    s_out = take(6)

    def num(part):
        return 1 if part == 1 else 0

    def y_start(pat):
        place, source, parts, base, _, kind, _ = pat

        def from_outer():
            for p in parts:
                for d in (1, -1):
                    send(source(p), place(0, 0, 1, p), kind, base + num(p), ydev(d))

        def from_inner():
            for p in parts:
                send(source(p), place(0, 0, 0, p), kind, base + 2 + num(p), ydev(2 * sigma))
                for h in (0, 1) if p is None else (p,):
                    send(source(h), place(0, 1, 0, h), kind, base + 6 + h, ydev(-2 * sigma))

        from_inner() if is_inner else from_outer()

    def x_send(pat, a, f, p):
        place, _, parts, _, base, _, kind = pat
        for d, slot in ((1, 1), (-1, 2)):
            s = base + ((slot - 1) * 4 + a * 2 + f) * len(parts) + num(p)
            send(place(0, a, f, p), place(slot, a, f, p), kind, s, xn[d])

    def y_near_other(pat, p):
        place, _, _, base, _, kind, _ = pat
        arrived(place(0, 0, 1, p), base + num(p))
        send(place(0, 0, 1, p), place(0, 1, 1, p), kind, base + 4 + num(p), ydev(-2 * sigma))
        x_send(pat, 0, 1, p)

    def y_near_own(pat):
        place, _, parts, base, _, kind, _ = pat
        for p in parts:
            if not is_inner:
                arrived(place(0, 0, 0, p), base + 2 + num(p))
                if p != 1:
                    send(place(0, 0, 0, 0), place(0, 1, 0, 0), kind, base + 6, ydev(-2 * sigma))
            x_send(pat, 0, 0, p)

    def y_far_own(pat):
        place, _, parts, base, _, kind, _ = pat
        for h in (1, 0):
            arrived(place(0, 1, 0, h), base + 6 + h)
            if not is_inner and h == 1:
                send(place(0, 1, 0, 1), place(0, 1, 0, 1), kind, base + 7, ydev(2 * sigma))
            if h in parts:
                x_send(pat, 1, 0, h)
        if None in parts:
            x_send(pat, 1, 0, None)

    def y_far_other(pat, p):
        place, _, _, base, _, _, _ = pat
        arrived(place(0, 1, 1, p), base + 4 + num(p))
        x_send(pat, 1, 1, p)

    def x_near(pat, a, f):
        place, _, parts, _, base, _, kind = pat
        for p in parts:
            for d, slot in ((1, 1), (-1, 2)):
                s = base + ((slot - 1) * 4 + a * 2 + f) * len(parts) + num(p)
                arrived(place(slot, a, f, p), s)
                if f == slot - 1:
                    s = base + (8 + a * 2 + f) * len(parts) + num(p)
                    send(place(slot, a, f, p), place(3, a, f, p), kind, s, xn[d])

    def x_far(pat, a, f):
        place, _, parts, _, base, _, _ = pat
        for p in parts:
            arrived(place(3, a, f, p), base + (8 + a * 2 + f) * len(parts) + num(p))

    cut = (feat // 2 + 15) // 16 * 16
    g_parts = {None: slice(None), 0: slice(0, cut), 1: slice(cut, feat)}
    p_parts = {None: (0, seq), 0: (0, seq // 2), 1: (seq // 2, seq)}

    def g_place(slot, a, f, part_=None):
        k, pos = HOME[slot, a]
        return g.at[k, f, g_parts[part_], pos * seq:(pos + 1) * seq]

    def p_place(slot, a, f, part_=None):
        lo, hi = p_parts[part_]
        return pa.at[slot, a * seq + lo:a * seq + hi, f * width:(f + 1) * width]

    def g_source(p):
        return gt.at[g_parts[p], :]

    def p_source(p):
        return paloc.at[slice(*p_parts[p]), :]

    gpat = (g_place, g_source, (0, 1), s_gy, s_gx, S_GY, S_GX)
    ppat = (p_place, p_source, (None,), s_py, s_px, S_PY, S_PX)

    def bt_place(f, c, i):
        return bt.at[f, pl.ds(pl.multiple_of(c * half + i * chunk, 16), chunk), :]

    def start():
        pltpu.make_async_copy(gt_hbm, gt, loc_sems.at[0]).wait()
        y_start(gpat)
        pltpu.make_async_copy(act_hbm, act.at[0, z], loc_sems.at[1]).wait()
        send(act.at[0, z], act.at[1, z], S_ACT, s_act0, ypart)

    def g_own():
        if is_inner:
            pltpu.make_async_copy(gt_hbm, own_block(), loc_sems.at[3]).wait()
        y_near_own(gpat)

    def bt_own():
        pltpu.make_async_copy(basis_hbm, raw, loc_sems.at[4]).wait()
        turned = raw[...].T
        bt[0, pl.ds(pl.multiple_of(core * half, 16), turned.shape[0]), :] = turned

    def bt_rows(f, lo, hi):
        return bt.at[f, pl.ds(pl.multiple_of(core * half + lo, 16), hi - lo), :]

    def bt_send(i, pieces=(0, 1)):
        split = chunk // 32 * 16
        for lo, hi in [((0, split), (split, chunk))[piece] for piece in pieces]:
            lo, hi = i * chunk + lo, i * chunk + hi
            send(bt_rows(0, lo, hi), bt_rows(1, lo, hi), S_BT, s_bt + 2 + i, ypart)
            send(bt_rows(0, lo, hi), bt_rows(0, lo, hi), S_BT, s_bt + i, sibling)

    def bt_forward(i):
        arrived(bt_place(1, core, i), s_bt + 2 + i)
        send(bt_place(1, core, i), bt_place(1, core, i), S_BT, s_bt + 4 + i, sibling)

    def bt_ready(i):
        arrived(bt_place(0, 1 - core, i), s_bt + i)
        arrived(bt_place(1, 1 - core, i), s_bt + 4 + i)

    def act_send(f, owner, k, tag):
        send(act.at[f, owner], act.at[f, owner], S_ACT, s_actz + tag, zn[k])

    def act_tag(f, d, dist):
        return f * 8 + (0 if d == 1 else 4) + dist - 1

    def act_first(f):
        if f == 1:
            arrived(act.at[1, z], s_act0)
        for dist in (2, 1):
            for d in (1, -1):
                act_send(f, z, d * dist, act_tag(f, d, dist))

    def act_wait(f, d, dist):
        arrived(act.at[f, (z + NZ - d * dist) % NZ], s_actz + act_tag(f, d, dist))

    def act_forward():
        for f in range(2):
            for d in (1, -1):
                act_wait(f, d, 2)
                owner = (z + NZ - 2 * d) % NZ
                if (f == 0) == (d == 1):
                    act_send(f, owner, 2 * d, act_tag(f, d, 4))
                act_send(f, owner, d, act_tag(f, d, 3))

    def act_rest():
        for dist in (1, 3, 4):
            for f in range(2):
                for d in (1, -1):
                    if dist < 4 or (f == 0) == (d == 1):
                        act_wait(f, d, dist)

    def project_acts():
        pltpu.make_async_copy(bin_hbm, binv, loc_sems.at[2]).wait()
        total = None
        for f in range(2):
            low = (yl if f == 0 else 1 - yl) * NZ
            rows = pl.ds(pl.multiple_of(low * width, 128), NZ * width)
            wide = jnp.concatenate([act[f, i] for i in range(NZ)], axis=1)
            t = jnp.dot(wide, binv[rows, :], preferred_element_type=F32)
            total = t if total is None else total + t
        paloc[...] = total.astype(BF16)

        if is_inner:
            pa[0, :seq, :width] = total.astype(BF16)

    def pa_start():
        y_start(ppat)

    def project(grp):
        a, i = grp // 2, grp % 2

        def body(c, carry):
            rows = pl.ds(pl.multiple_of(c * half + i * chunk, 16), chunk)
            for pair in range(2):
                cols = slice(2 * pair * seq, 2 * (pair + 1) * seq)
                t = jnp.dot(bt[0, rows, :], g[a, 0, :, cols], preferred_element_type=F32)
                t = t + jnp.dot(bt[1, rows, :], g[a, 1, :, cols], preferred_element_type=F32)
                t = t.astype(BF16)
                part[grp, c * 4 + 2 * pair] = t[:, :seq]
                part[grp, c * 4 + 2 * pair + 1] = t[:, seq:]
            return carry

        lax.fori_loop(0, 2, body, 0)

    def rlen(grp, d):
        return 4 if (grp % 2 == 0) == (d == 1) else 3

    def rs_slot(d, k):
        return (0 if d == 1 else 4) + k

    def rs_step(grp, k):
        for d in (1, -1):
            n = rlen(grp, d)
            if k < n:
                j = (z + NZ + d * (n - k)) % NZ
                if k == 0:
                    src = part.at[grp, j]
                else:
                    slot = rs_slot(d, k - 1)
                    src = rsb.at[grp, slot]
                    arrived(src, s_rs + grp * 8 + slot)
                    rsb[grp, slot] = (rsb[grp, slot].astype(F32) + part[grp, j].astype(F32)).astype(BF16)
                s = s_rs + grp * 8 + rs_slot(d, k)
                send(src, rsb.at[grp, rs_slot(d, k)], S_RS, s, zn[d])

    def rs_two_first(grp):
        for d in (1, -1):
            for dist, hop, slot in ((4, 2, 2), (3, 1, 1), (1, 1, 0)):
                if dist <= rlen(grp, d):
                    slot = rs_slot(d, slot)
                    send(part.at[grp, (z + NZ + d * dist) % NZ], rsb.at[grp, slot], S_RS, s_rs + grp * 8 + slot, zn[d * hop])

    def rs_two_middle(grp):
        for d in (1, -1):
            total = part[grp, (z + NZ + 2 * d) % NZ].astype(F32)
            for k in range(1, rlen(grp, d) - 1):
                slot = rs_slot(d, k)
                arrived(rsb.at[grp, slot], s_rs + grp * 8 + slot)
                total = total + rsb[grp, slot].astype(F32)
            rsb[grp, rs_slot(d, 1)] = total.astype(BF16)
            slot = rs_slot(d, 3)
            send(rsb.at[grp, rs_slot(d, 1)], rsb.at[grp, slot], S_RS, s_rs + grp * 8 + slot, zn[2 * d])

    def pg_place(grp, j):
        return pg.at[grp, pl.ds(pl.multiple_of(j * chunk, 16), chunk), :]

    def ag_sem(grp, d, k):
        return s_ag + grp * 8 + rs_slot(d, k)

    def rs_last(grp, two_steps=False, ag_two_steps=False):
        total = part[grp, z].astype(F32)
        for d in (1, -1):
            for k in (0, 3) if two_steps else (rlen(grp, d) - 1,):
                slot = rs_slot(d, k)
                arrived(rsb.at[grp, slot], s_rs + grp * 8 + slot)
                total = total + rsb[grp, slot].astype(F32)
        pg[grp, pl.ds(pl.multiple_of(z * chunk, 16), chunk), :] = total.astype(BF16)
        for dist in (2, 1) if ag_two_steps else (1,):
            for d in (1, -1):
                send(pg_place(grp, z), pg_place(grp, z), S_AG, ag_sem(grp, d, dist - 1), zn[d * dist])

    def ag_wait(grp, d, dist):
        j = (z + NZ - d * dist) % NZ
        arrived(pg_place(grp, j), ag_sem(grp, d, dist - 1))
        return pg_place(grp, j)

    def ag_step(grp, k):
        for d in (1, -1):
            n = rlen(grp, d)
            if k <= n:
                piece = ag_wait(grp, d, k)
                if k < n:
                    send(piece, piece, S_AG, ag_sem(grp, d, k), zn[d])

    def ag_two_middle(grp):
        for d in (1, -1):
            piece = ag_wait(grp, d, 2)
            if rlen(grp, d) == 4:
                send(piece, piece, S_AG, ag_sem(grp, d, 3), zn[2 * d])
            send(piece, piece, S_AG, ag_sem(grp, d, 2), zn[d])

    def ag_two_last(grp):
        for dist in (1, 3, 4):
            for d in (1, -1):
                if dist <= rlen(grp, d):
                    ag_wait(grp, d, dist)

    def squares(grp, lo, hi):
        a, i = grp // 2, grp % 2

        def body(c, carry):
            rows = pl.ds(pl.multiple_of(c * half + i * chunk, 16), chunk)
            total = None if a == 0 else acc[rows, lo:hi]
            for pos, (slot, far) in enumerate(SETS[a]):
                lhs = pg[grp, pl.ds(pl.multiple_of((c * 4 + pos) * chunk, 16), chunk), :]
                t = jnp.dot(lhs, pa[slot, far * seq:(far + 1) * seq, lo:hi], preferred_element_type=F32)
                total = t * t if total is None else total + t * t
            acc[rows, lo:hi] = total
            return carry

        lax.fori_loop(0, 2, body, 0)

    spans = (slice(0, width), slice(width, 2 * width))

    def acc_rows(c, i):
        return pl.ds(pl.multiple_of(c * half + i * chunk, 8), chunk)

    def out_core(i, f):
        dst = xrecv.at[i * chunk:(i + 1) * chunk, spans[f]]
        send(acc.at[acc_rows(1 - core, i), spans[f]], dst, S_OC, s_out + 2 * i + f, sibling)

    def out_y(i):
        rows = slice(i * chunk, (i + 1) * chunk)
        arrived(xrecv.at[rows, spans[1]], s_out + 2 * i + 1)
        ysend[rows, :] = (acc[acc_rows(core, i), spans[1]] + xrecv[rows, spans[1]]).astype(BF16)
        send(ysend.at[rows, :], yrecv.at[rows, :], S_OY, s_out + 4 + i, ypart)

    def out_y_of(i, c):
        pl.when(core == c)(lambda: out_y(i))

    def out_last(i):
        rows = slice(i * chunk, (i + 1) * chunk)
        n = min(chunk, out_ref.shape[0] - i * chunk)
        arrived(xrecv.at[rows, spans[0]], s_out + 2 * i)
        own = acc[acc_rows(core, i), spans[0]] + xrecv[rows, spans[0]]
        arrived(yrecv.at[rows, :], s_out + 4 + i)
        own = (own + yrecv[rows, :].astype(F32)) * (1.0 / 4096.0)
        out_ref[i * chunk:i * chunk + n, :] = own[:n]

    steps = []

    def at(t_inner, t_outer, fn, *args):
        steps.append((t_inner if is_inner else t_outer, len(steps), functools.partial(fn, *args)))

    at(0, 0, start)
    at(0.04, 11, g_own)
    at(0.05, 0.05, act_first, 0)
    at(0.3, 0.3, bt_own)
    at(0.35, 6.4, bt_send, 0, (0,))
    at(0.35, 11.2, bt_send, 0, (1,))
    at(0.36, 11.25, bt_send, 1)
    at(4, 4.5, y_near_other, gpat, 0)
    at(5.8, 6.3, y_near_other, gpat, 1)
    at(6.5, 15.5, x_near, gpat, 0, 0)
    at(15.45, 11.1, y_far_own, gpat)
    at(10.5, 12, x_near, gpat, 0, 1)
    at(11, 13, y_far_other, gpat, 0)
    at(12.5, 14.5, y_far_other, gpat, 1)
    at(12.6, 12.1, act_first, 1)
    at(15.3, 17, act_forward)
    at(15.5, 18.2, bt_forward, 0)
    at(28, 22.42, x_far, gpat, 0, 0)
    at(28, 22.42, x_far, gpat, 0, 1)
    at(15.4, 18.8, x_near, gpat, 1, 1)
    at(20.9, 18.5, x_near, gpat, 1, 0)
    at(18.5, 18.6, bt_ready, 0)
    at(18.6, 18.6, project, 0)
    at(18.6, 18.6, rs_two_first, 0)
    at(20.96, 19, rs_two_middle, 0)
    at(28.3, 28.3, rs_last, 0, True)
    for k in range(1, 5):
        at(28.9 + 3.9 * k, 28.9 + 3.9 * k, ag_step, 0, k)
    at(25.1, 22.41, act_rest)
    at(25.1, 22.41, project_acts)
    at(25.1, 22.41, pa_start)
    at(20.95, 18.7, bt_forward, 1)
    at(25, 22.4, bt_ready, 1)
    at(25, 22.4, project, 1)
    at(25, 22.4, rs_step, 1, 0)
    at(28, 28, x_far, gpat, 1, 0)
    at(28, 28, x_far, gpat, 1, 1)
    for grp in (2, 3):
        at(28 + grp / 20, 28 + grp / 20, project, grp)
        at(28 + grp / 20, 28 + grp / 20, rs_step, grp, 0)
    at(25.2, 33.46, y_near_own, ppat)
    at(33.45, 33.45, y_near_other, ppat, None)
    at(41.1, 33.47, y_far_own, ppat)
    at(41, 41, y_far_other, ppat, None)
    for i, (a, f) in enumerate(((0, 0), (0, 1), (1, 1), (1, 0))):
        t = (43, 43, 47.4, 47.4)[i]
        at(t, t, x_near, ppat, a, f)
        t = (48, 48, 54.8, 54.8)[i]
        at(t, t, x_far, ppat, a, f)
    for grp, t_in, t_out, t_last in (
        (1, (28.25, 33.5, 37.5), (28.25, 33.5, 37.5), 41),
        (2, (32, 33.4, 37.4), (32, 33.4, 37.4), 40.9),
        (3, (32.1, 34, 38), (32.1, 34, 38), 41.5),
    ):
        for k in range(3):
            at(t_in[k], t_out[k], rs_step, grp, k + 1)
        two = grp in ()
        at(t_last, t_last, rs_last, grp, False, two)
        if two:
            at(t_last + 4.9, t_last + 4.9, ag_two_middle, grp)
            at(t_last + 9.9, t_last + 9.9, ag_two_last, grp)
        else:
            for k in range(1, 5):
                at(t_last + 4 * k, t_last + 4 * k, ag_step, grp, k)
    at(53, 53, squares, 0, 0, 2 * width)
    at(56.95, 56.95, squares, 2, 0, 2 * width)
    at(56.95, 56.95, out_core, 0, 1)
    at(56.95, 56.95, out_core, 0, 0)
    at(57.1, 57.1, squares, 1, 0, 2 * width)
    at(57.05, 57.05, out_y_of, 0, 0)
    at(59.15, 59.15, out_y_of, 0, 1)
    at(59, 59, squares, 3, width, 2 * width)
    at(59, 59, out_core, 1, 1)
    at(59.1, 59.1, squares, 3, 0, width)
    at(59.2, 59.2, out_core, 1, 0)
    at(61, 61, out_y, 1)
    at(62, 62, out_last, 0)
    at(63, 63, out_last, 1)

    def drain():
        def sent(ref, kind):
            pltpu.make_async_copy(ref, ref, send_sems.at[kind]).wait()

        blocks = 3 if is_inner else 4
        sent(g.at[0, 0, :, :blocks * seq], S_GY)
        sent(act.at[0, :blocks], S_PY)
        sent(g.at[:, :, :, seq:], S_GX)
        sent(pa.at[1:], S_PX)
        sent(binv.at[:15 * seq, :], S_ACT)
        sent(bt.at[:, :3 * chunk, :], S_BT)
        sent(rsb.at[:, :7], S_RS)
        sent(rsb.at[:, :7], S_AG)
        sent(xrecv, S_OC)
        sent(yrecv, S_OY)

    at(999, 999, drain)
    assert counter[0] == recv_sems.shape[0]
    for _, _, fn in sorted(steps, key=lambda s: (s[0], s[1])):
        fn()


def shards(activations, gradients, basis_in, basis_out):
    seq, feat = gradients.shape[1:]
    cols = basis_out.shape[1]
    width = basis_in.shape[1]
    half = (cols + 31) // 32 * 32
    chunk = half // 2
    gt = gradients[0].T
    dims = (feat, seq, half, chunk, width)
    return pl.pallas_call(
        functools.partial(kernel, dims),
        out_shape=jax.ShapeDtypeStruct((cols, width), F32),
        in_specs=[pl.BlockSpec(memory_space=pltpu.HBM)] * 4,
        out_specs=pl.BlockSpec(memory_space=pltpu.VMEM),
        scratch_shapes=[
            pltpu.VMEM((feat, cols), BF16),
            pltpu.VMEM((NYL, 2 * half, feat), BF16),
            pltpu.VMEM((feat, seq), BF16),
            pltpu.VMEM((2, NYL, feat, 4 * seq), BF16),
            pltpu.VMEM((NYL, NZ, seq, width), BF16),
            pltpu.VMEM(basis_in.shape, BF16),
            pltpu.VMEM((seq, width), BF16),
            pltpu.VMEM((4, 2 * seq, 2 * width), BF16),
            pltpu.VMEM((4, NZ, chunk, seq), BF16),
            pltpu.VMEM((4, NZ, chunk, seq), BF16),
            pltpu.VMEM((4, NZ * chunk, seq), BF16),
            pltpu.VMEM((2 * half, 2 * width), F32),
            pltpu.VMEM((half, 2 * width), F32),
            pltpu.VMEM((half, width), BF16),
            pltpu.VMEM((half, width), BF16),
            pltpu.SemaphoreType.DMA((10,)),
            pltpu.SemaphoreType.DMA((145,)),
            pltpu.SemaphoreType.DMA((5,)),
        ],
        compiler_params=pltpu.CompilerParams(
            collective_id=0, has_side_effects=True, vmem_limit_bytes=40 * 1024 * 1024
        ),
        name="ekfac",
    )(*[pltpu.with_memory_space_constraint(v, pltpu.HBM) for v in (basis_out, gt, activations[0], basis_in)])


def solution(mesh):
    return jax.shard_map(
        shards,
        mesh=mesh,
        in_specs=(P("dp", None, "mp"), P("dp", None, "mp"), P(None, "mp"), P("mp", "dp")),
        out_specs=P("dp", "mp"),
        check_vma=False,
    )
```

```python
import functools

import jax
import jax.numpy as jnp
from jax import lax
from jax.experimental import pallas as pl
from jax.experimental.pallas import tpu as pltpu
from jax.sharding import PartitionSpec as P

MESH = pl.DeviceIdType.MESH
NX, NYH, NYL, NZ = 4, 4, 2, 8
F32, BF16 = jnp.float32, jnp.bfloat16
SETS = (((0, 0), (1, 0), (2, 0), (0, 1)), ((3, 0), (1, 1), (2, 1), (3, 1)))
HOME = {key: (k, pos) for k, keys in enumerate(SETS) for pos, key in enumerate(keys)}


def kernel(
    dims, basis_hbm, gt_hbm, act_hbm, bin_hbm, out_ref,
    raw, bt, gt, g, act, binv, paloc, pa, part, rsb, pg, acc, xrecv, ysend, yrecv,
    send_sems, recv_sems, loc_sems,
):
    feat, seq, half, chunk, width = dims
    dp, mp = lax.axis_index("dp"), lax.axis_index("mp")
    core, x, yh = dp % 2, (dp // 2) % NX, dp // (2 * NX)
    yl, z = mp // NZ, mp % NZ

    def dev(yh_=None, x_=None, c_=None, yl_=None, z_=None):
        yh_ = yh if yh_ is None else yh_
        x_ = x if x_ is None else x_
        c_ = core if c_ is None else c_
        yl_ = yl if yl_ is None else yl_
        z_ = z if z_ is None else z_
        return ((yh_ * NX + x_) * 2 + c_, yl_ * NZ + z_)

    sibling = dev(c_=1 - core)
    ypart = dev(yl_=1 - yl)
    xn = {1: dev(x_=(x + 1) % NX), -1: dev(x_=(x + NX - 1) % NX)}
    zn = {k: dev(z_=(z + NZ + k) % NZ) for k in (1, -1, 2, -2)}

    y = yh * NYL + yl
    ny = NYH * NYL

    def ydev(k):
        yy = (y + ny + k) % ny
        return dev(yh_=yy // NYL, yl_=yy % NYL)

    sigma = 1 - 2 * (yh % 2)
    inner = yl == yh % 2
    outer = yl != yh % 2

    def own_block():
        return g.at[0, 0, :, :seq]

    pltpu.make_async_copy(gt_hbm, gt, loc_sems.at[0]).start()
    pltpu.make_async_copy(act_hbm, act.at[0, z], loc_sems.at[1]).start()
    pltpu.make_async_copy(basis_hbm, raw, loc_sems.at[4]).start()
    pltpu.make_async_copy(bin_hbm, binv, loc_sems.at[2]).start()
    pl.when(inner)(lambda: pltpu.make_async_copy(gt_hbm, own_block(), loc_sems.at[3]).start())

    barrier = pltpu.get_barrier_semaphore()
    peers = [sibling, xn[1], xn[-1], zn[1], zn[-1], zn[2], zn[-2], ydev(1), ydev(-1), ydev(2), ydev(-2)]
    for peer in peers:
        pl.semaphore_signal(barrier, inc=1, device_id=peer, device_id_type=MESH)
    pl.semaphore_wait(barrier, len(peers))

    refs = (basis_hbm, gt_hbm, act_hbm, bin_hbm, out_ref, raw, bt, gt, g, act, binv, paloc, pa, part, rsb, pg, acc,
            xrecv, ysend, yrecv, send_sems, recv_sems, loc_sems)
    where = (core, yl, z, sigma, sibling, ypart, xn, zn, ydev, own_block)
    pl.when(inner)(lambda: program(True, dims, where, *refs))
    pl.when(outer)(lambda: program(False, dims, where, *refs))


def program(
    is_inner, dims, where, basis_hbm, gt_hbm, act_hbm, bin_hbm, out_ref, raw, bt, gt, g, act, binv, paloc, pa, part,
    rsb, pg, acc, xrecv, ysend, yrecv, send_sems, recv_sems, loc_sems,
):
    feat, seq, half, chunk, width = dims
    core, yl, z, sigma, sibling, ypart, xn, zn, ydev, own_block = where
    counter = [0]

    def take(n=1):
        base = counter[0]
        counter[0] += n
        return base

    S_GY, S_GX, S_PY, S_PX, S_ACT, S_BT, S_RS, S_AG, S_OC, S_OY = range(10)

    def send(src, dst, kind, rsem, to):
        pltpu.make_async_remote_copy(
            src_ref=src, dst_ref=dst, send_sem=send_sems.at[kind], recv_sem=recv_sems.at[rsem],
            device_id=to, device_id_type=MESH,
        ).start()

    def arrived(dst, rsem):
        pltpu.make_async_copy(dst, dst, recv_sems.at[rsem]).wait()

    s_bt = take(6)
    s_act0 = take(1)
    s_gy, s_gx = take(8), take(24)
    s_py, s_px = take(8), take(12)
    s_actz = take(16)
    s_rs, s_ag = take(32), take(32)
    s_out = take(6)

    def num(part):
        return 1 if part == 1 else 0

    def y_start(pat):
        place, source, parts, base, _, kind, _ = pat

        def from_outer():
            for p in parts:
                for d in (1, -1):
                    send(source(p), place(0, 0, 1, p), kind, base + num(p), ydev(d))

        def from_inner():
            for p in parts:
                send(source(p), place(0, 0, 0, p), kind, base + 2 + num(p), ydev(2 * sigma))
                for h in (0, 1) if p is None else (p,):
                    send(source(h), place(0, 1, 0, h), kind, base + 6 + h, ydev(-2 * sigma))

        from_inner() if is_inner else from_outer()

    def x_send(pat, a, f, p):
        place, _, parts, _, base, _, kind = pat
        for d, slot in ((1, 1), (-1, 2)):
            s = base + ((slot - 1) * 4 + a * 2 + f) * len(parts) + num(p)
            send(place(0, a, f, p), place(slot, a, f, p), kind, s, xn[d])

    def y_near_other(pat, p):
        place, _, _, base, _, kind, _ = pat
        arrived(place(0, 0, 1, p), base + num(p))
        send(place(0, 0, 1, p), place(0, 1, 1, p), kind, base + 4 + num(p), ydev(-2 * sigma))
        x_send(pat, 0, 1, p)

    def y_near_own(pat):
        place, _, parts, base, _, kind, _ = pat
        for p in parts:
            if not is_inner:
                arrived(place(0, 0, 0, p), base + 2 + num(p))
                if p != 1:
                    send(place(0, 0, 0, 0), place(0, 1, 0, 0), kind, base + 6, ydev(-2 * sigma))
            x_send(pat, 0, 0, p)

    def y_far_own(pat):
        place, _, parts, base, _, kind, _ = pat
        for h in (1, 0):
            arrived(place(0, 1, 0, h), base + 6 + h)
            if not is_inner and h == 1:
                send(place(0, 1, 0, 1), place(0, 1, 0, 1), kind, base + 7, ydev(2 * sigma))
            if h in parts:
                x_send(pat, 1, 0, h)
        if None in parts:
            x_send(pat, 1, 0, None)

    def y_far_other(pat, p):
        place, _, _, base, _, _, _ = pat
        arrived(place(0, 1, 1, p), base + 4 + num(p))
        x_send(pat, 1, 1, p)

    def x_near(pat, a, f):
        place, _, parts, _, base, _, kind = pat
        for p in parts:
            for d, slot in ((1, 1), (-1, 2)):
                s = base + ((slot - 1) * 4 + a * 2 + f) * len(parts) + num(p)
                arrived(place(slot, a, f, p), s)
                if f == slot - 1:
                    s = base + (8 + a * 2 + f) * len(parts) + num(p)
                    send(place(slot, a, f, p), place(3, a, f, p), kind, s, xn[d])

    def x_far(pat, a, f):
        place, _, parts, _, base, _, _ = pat
        for p in parts:
            arrived(place(3, a, f, p), base + (8 + a * 2 + f) * len(parts) + num(p))

    cut = (feat // 2 + 15) // 16 * 16
    g_parts = {None: slice(None), 0: slice(0, cut), 1: slice(cut, feat)}
    p_parts = {None: (0, seq), 0: (0, seq // 2), 1: (seq // 2, seq)}

    def g_place(slot, a, f, part_=None):
        k, pos = HOME[slot, a]
        return g.at[k, f, g_parts[part_], pos * seq:(pos + 1) * seq]

    def p_place(slot, a, f, part_=None):
        lo, hi = p_parts[part_]
        return pa.at[slot, a * seq + lo:a * seq + hi, f * width:(f + 1) * width]

    def g_source(p):
        return gt.at[g_parts[p], :]

    def p_source(p):
        return paloc.at[slice(*p_parts[p]), :]

    gpat = (g_place, g_source, (0, 1), s_gy, s_gx, S_GY, S_GX)
    ppat = (p_place, p_source, (None,), s_py, s_px, S_PY, S_PX)

    def bt_place(f, c, i):
        return bt.at[f, pl.ds(pl.multiple_of(c * half + i * chunk, 16), chunk), :]

    def start():
        pltpu.make_async_copy(gt_hbm, gt, loc_sems.at[0]).wait()
        y_start(gpat)
        pltpu.make_async_copy(act_hbm, act.at[0, z], loc_sems.at[1]).wait()
        send(act.at[0, z], act.at[1, z], S_ACT, s_act0, ypart)

    def g_own():
        if is_inner:
            pltpu.make_async_copy(gt_hbm, own_block(), loc_sems.at[3]).wait()
        y_near_own(gpat)

    def bt_own():
        pltpu.make_async_copy(basis_hbm, raw, loc_sems.at[4]).wait()
        turned = raw[...].T
        bt[0, pl.ds(pl.multiple_of(core * half, 16), turned.shape[0]), :] = turned

    def bt_rows(f, lo, hi):
        return bt.at[f, pl.ds(pl.multiple_of(core * half + lo, 16), hi - lo), :]

    def bt_send(i, pieces=(0, 1)):
        split = chunk // 32 * 16
        for lo, hi in [((0, split), (split, chunk))[piece] for piece in pieces]:
            lo, hi = i * chunk + lo, i * chunk + hi
            send(bt_rows(0, lo, hi), bt_rows(1, lo, hi), S_BT, s_bt + 2 + i, ypart)
            send(bt_rows(0, lo, hi), bt_rows(0, lo, hi), S_BT, s_bt + i, sibling)

    def bt_forward(i):
        arrived(bt_place(1, core, i), s_bt + 2 + i)
        send(bt_place(1, core, i), bt_place(1, core, i), S_BT, s_bt + 4 + i, sibling)

    def bt_ready(i):
        arrived(bt_place(0, 1 - core, i), s_bt + i)
        arrived(bt_place(1, 1 - core, i), s_bt + 4 + i)

    def act_send(f, owner, k, tag):
        send(act.at[f, owner], act.at[f, owner], S_ACT, s_actz + tag, zn[k])

    def act_tag(f, d, dist):
        return f * 8 + (0 if d == 1 else 4) + dist - 1

    def act_first(f):
        if f == 1:
            arrived(act.at[1, z], s_act0)
        for dist in (2, 1):
            for d in (1, -1):
                act_send(f, z, d * dist, act_tag(f, d, dist))

    def act_wait(f, d, dist):
        arrived(act.at[f, (z + NZ - d * dist) % NZ], s_actz + act_tag(f, d, dist))

    def act_forward():
        for f in range(2):
            for d in (1, -1):
                act_wait(f, d, 2)
                owner = (z + NZ - 2 * d) % NZ
                if (f == 0) == (d == 1):
                    act_send(f, owner, 2 * d, act_tag(f, d, 4))
                act_send(f, owner, d, act_tag(f, d, 3))

    def act_rest():
        for dist in (1, 3, 4):
            for f in range(2):
                for d in (1, -1):
                    if dist < 4 or (f == 0) == (d == 1):
                        act_wait(f, d, dist)

    def project_acts():
        pltpu.make_async_copy(bin_hbm, binv, loc_sems.at[2]).wait()
        total = None
        for f in range(2):
            low = (yl if f == 0 else 1 - yl) * NZ
            rows = pl.ds(pl.multiple_of(low * width, 128), NZ * width)
            wide = jnp.concatenate([act[f, i] for i in range(NZ)], axis=1)
            t = jnp.dot(wide, binv[rows, :], preferred_element_type=F32)
            total = t if total is None else total + t
        paloc[...] = total.astype(BF16)

        if is_inner:
            pa[0, :seq, :width] = total.astype(BF16)

    def pa_start():
        y_start(ppat)

    def project(grp):
        a, i = grp // 2, grp % 2

        def body(c, carry):
            rows = pl.ds(pl.multiple_of(c * half + i * chunk, 16), chunk)
            for pair in range(2):
                cols = slice(2 * pair * seq, 2 * (pair + 1) * seq)
                t = jnp.dot(bt[0, rows, :], g[a, 0, :, cols], preferred_element_type=F32)
                t = t + jnp.dot(bt[1, rows, :], g[a, 1, :, cols], preferred_element_type=F32)
                t = t.astype(BF16)
                part[grp, c * 4 + 2 * pair] = t[:, :seq]
                part[grp, c * 4 + 2 * pair + 1] = t[:, seq:]
            return carry

        lax.fori_loop(0, 2, body, 0)

    def rlen(grp, d):
        return 4 if (grp % 2 == 0) == (d == 1) else 3

    def rs_slot(d, k):
        return (0 if d == 1 else 4) + k

    def rs_step(grp, k):
        for d in (1, -1):
            n = rlen(grp, d)
            if k < n:
                j = (z + NZ + d * (n - k)) % NZ
                if k == 0:
                    src = part.at[grp, j]
                else:
                    slot = rs_slot(d, k - 1)
                    src = rsb.at[grp, slot]
                    arrived(src, s_rs + grp * 8 + slot)
                    rsb[grp, slot] = (rsb[grp, slot].astype(F32) + part[grp, j].astype(F32)).astype(BF16)
                s = s_rs + grp * 8 + rs_slot(d, k)
                send(src, rsb.at[grp, rs_slot(d, k)], S_RS, s, zn[d])

    def rs_two_first(grp):
        for d in (1, -1):
            for dist, hop, slot in ((4, 2, 2), (3, 1, 1), (1, 1, 0)):
                if dist <= rlen(grp, d):
                    slot = rs_slot(d, slot)
                    send(part.at[grp, (z + NZ + d * dist) % NZ], rsb.at[grp, slot], S_RS, s_rs + grp * 8 + slot, zn[d * hop])

    def rs_two_middle(grp):
        for d in (1, -1):
            total = part[grp, (z + NZ + 2 * d) % NZ].astype(F32)
            for k in range(1, rlen(grp, d) - 1):
                slot = rs_slot(d, k)
                arrived(rsb.at[grp, slot], s_rs + grp * 8 + slot)
                total = total + rsb[grp, slot].astype(F32)
            rsb[grp, rs_slot(d, 1)] = total.astype(BF16)
            slot = rs_slot(d, 3)
            send(rsb.at[grp, rs_slot(d, 1)], rsb.at[grp, slot], S_RS, s_rs + grp * 8 + slot, zn[2 * d])

    def pg_place(grp, j):
        return pg.at[grp, pl.ds(pl.multiple_of(j * chunk, 16), chunk), :]

    def ag_sem(grp, d, k):
        return s_ag + grp * 8 + rs_slot(d, k)

    def rs_last(grp, two_steps=False, ag_two_steps=False):
        total = part[grp, z].astype(F32)
        for d in (1, -1):
            for k in (0, 3) if two_steps else (rlen(grp, d) - 1,):
                slot = rs_slot(d, k)
                arrived(rsb.at[grp, slot], s_rs + grp * 8 + slot)
                total = total + rsb[grp, slot].astype(F32)
        pg[grp, pl.ds(pl.multiple_of(z * chunk, 16), chunk), :] = total.astype(BF16)
        for dist in (2, 1) if ag_two_steps else (1,):
            for d in (1, -1):
                send(pg_place(grp, z), pg_place(grp, z), S_AG, ag_sem(grp, d, dist - 1), zn[d * dist])

    def ag_wait(grp, d, dist):
        j = (z + NZ - d * dist) % NZ
        arrived(pg_place(grp, j), ag_sem(grp, d, dist - 1))
        return pg_place(grp, j)

    def ag_step(grp, k):
        for d in (1, -1):
            n = rlen(grp, d)
            if k <= n:
                piece = ag_wait(grp, d, k)
                if k < n:
                    send(piece, piece, S_AG, ag_sem(grp, d, k), zn[d])

    def ag_two_middle(grp):
        for d in (1, -1):
            piece = ag_wait(grp, d, 2)
            if rlen(grp, d) == 4:
                send(piece, piece, S_AG, ag_sem(grp, d, 3), zn[2 * d])
            send(piece, piece, S_AG, ag_sem(grp, d, 2), zn[d])

    def ag_two_last(grp):
        for dist in (1, 3, 4):
            for d in (1, -1):
                if dist <= rlen(grp, d):
                    ag_wait(grp, d, dist)

    def squares(grp, lo, hi, whose=None):
        a, i = grp // 2, grp % 2

        def body(c, carry):
            rows = pl.ds(pl.multiple_of(c * half + i * chunk, 16), chunk)
            total = None if a == 0 else acc[rows, lo:hi]
            for pos, (slot, far) in enumerate(SETS[a]):
                lhs = pg[grp, pl.ds(pl.multiple_of((c * 4 + pos) * chunk, 16), chunk), :]
                t = jnp.dot(lhs, pa[slot, far * seq:(far + 1) * seq, lo:hi], preferred_element_type=F32)
                total = t * t if total is None else total + t * t
            acc[rows, lo:hi] = total
            return carry

        if whose is None:
            lax.fori_loop(0, 2, body, 0)
        else:
            body(core if whose else 1 - core, 0)

    spans = (slice(0, width), slice(width, 2 * width))

    def acc_rows(c, i):
        return pl.ds(pl.multiple_of(c * half + i * chunk, 8), chunk)

    def out_core(i, f):
        dst = xrecv.at[i * chunk:(i + 1) * chunk, spans[f]]
        send(acc.at[acc_rows(1 - core, i), spans[f]], dst, S_OC, s_out + 2 * i + f, sibling)

    def out_y(i):
        rows = slice(i * chunk, (i + 1) * chunk)
        arrived(xrecv.at[rows, spans[1]], s_out + 2 * i + 1)
        ysend[rows, :] = (acc[acc_rows(core, i), spans[1]] + xrecv[rows, spans[1]]).astype(BF16)
        send(ysend.at[rows, :], yrecv.at[rows, :], S_OY, s_out + 4 + i, ypart)

    def out_y_of(i, c):
        pl.when(core == c)(lambda: out_y(i))

    def out_last(i):
        rows = slice(i * chunk, (i + 1) * chunk)
        n = min(chunk, out_ref.shape[0] - i * chunk)
        arrived(xrecv.at[rows, spans[0]], s_out + 2 * i)
        own = acc[acc_rows(core, i), spans[0]] + xrecv[rows, spans[0]]
        arrived(yrecv.at[rows, :], s_out + 4 + i)
        own = (own + yrecv[rows, :].astype(F32)) * (1.0 / 4096.0)
        out_ref[i * chunk:i * chunk + n, :] = own[:n]

    steps = []

    def at(t_inner, t_outer, fn, *args):
        steps.append((t_inner if is_inner else t_outer, len(steps), functools.partial(fn, *args)))

    at(0, 0, start)
    at(0.04, 11, g_own)
    at(0.05, 0.05, act_first, 0)
    at(0.3, 0.3, bt_own)
    at(0.35, 6.4, bt_send, 0, (0,))
    at(0.35, 11.2, bt_send, 0, (1,))
    at(0.36, 11.25, bt_send, 1)
    at(4, 4.5, y_near_other, gpat, 0)
    at(5.8, 6.3, y_near_other, gpat, 1)
    at(6.5, 15.5, x_near, gpat, 0, 0)
    at(15.45, 11.1, y_far_own, gpat)
    at(10.5, 12, x_near, gpat, 0, 1)
    at(11, 13, y_far_other, gpat, 0)
    at(12.5, 14.5, y_far_other, gpat, 1)
    at(12.6, 12.1, act_first, 1)
    at(15.3, 17, act_forward)
    at(15.5, 18.2, bt_forward, 0)
    at(28, 22.42, x_far, gpat, 0, 0)
    at(28, 22.42, x_far, gpat, 0, 1)
    at(15.4, 18.8, x_near, gpat, 1, 1)
    at(20.9, 18.5, x_near, gpat, 1, 0)
    at(18.5, 18.6, bt_ready, 0)
    at(18.6, 18.6, project, 0)
    at(18.6, 18.6, rs_two_first, 0)
    at(20.96, 19, rs_two_middle, 0)
    at(28.3, 28.3, rs_last, 0, True)
    for k in range(1, 5):
        at(28.9 + 3.9 * k, 28.9 + 3.9 * k, ag_step, 0, k)
    at(25.1, 22.41, act_rest)
    at(25.1, 22.41, project_acts)
    at(25.1, 22.41, pa_start)
    at(20.95, 18.7, bt_forward, 1)
    at(25, 22.4, bt_ready, 1)
    at(25, 22.4, project, 1)
    at(25, 22.4, rs_step, 1, 0)
    at(28, 28, x_far, gpat, 1, 0)
    at(28, 28, x_far, gpat, 1, 1)
    for grp in (2, 3):
        at(28 + grp / 20, 28 + grp / 20, project, grp)
        at(28 + grp / 20, 28 + grp / 20, rs_step, grp, 0)
    at(25.2, 33.46, y_near_own, ppat)
    at(33.45, 33.45, y_near_other, ppat, None)
    at(41.1, 33.47, y_far_own, ppat)
    at(41, 41, y_far_other, ppat, None)
    for i, (a, f) in enumerate(((0, 0), (0, 1), (1, 1), (1, 0))):
        t = (43, 43, 47.4, 47.4)[i]
        at(t, t, x_near, ppat, a, f)
        t = (48, 48, 54.8, 54.8)[i]
        at(t, t, x_far, ppat, a, f)
    for grp, t_in, t_out, t_last in (
        (1, (28.25, 33.5, 37.5), (28.25, 33.5, 37.5), 41),
        (2, (32, 33.4, 37.4), (32, 33.4, 37.4), 40.9),
        (3, (32.1, 34, 38), (32.1, 34, 38), 41.5),
    ):
        for k in range(3):
            at(t_in[k], t_out[k], rs_step, grp, k + 1)
        two = grp in ()
        at(t_last, t_last, rs_last, grp, False, two)
        if two:
            at(t_last + 4.9, t_last + 4.9, ag_two_middle, grp)
            at(t_last + 9.9, t_last + 9.9, ag_two_last, grp)
        else:
            for k in range(1, 5):
                at(t_last + 4 * k, t_last + 4 * k, ag_step, grp, k)
    at(53, 53, squares, 0, 0, 2 * width)
    at(56.95, 56.95, squares, 2, 0, 2 * width)
    at(56.95, 56.95, out_core, 0, 1)
    at(56.95, 56.95, out_core, 0, 0)
    at(57.1, 57.1, squares, 1, 0, 2 * width)
    at(57.05, 57.05, out_y_of, 0, 0)
    at(59, 59, squares, 3, width, 2 * width, 0)
    at(59, 59, out_core, 1, 1)
    at(59, 59, squares, 3, 0, width, 0)
    at(59, 59, out_core, 1, 0)
    at(59, 59, squares, 3, width, 2 * width, 1)
    at(59, 59, out_y_of, 0, 1)
    at(61.1, 61.1, squares, 3, 0, width, 1)
    at(61, 61, out_y, 1)
    at(62, 62, out_last, 0)
    at(63, 63, out_last, 1)

    def drain():
        def sent(ref, kind):
            pltpu.make_async_copy(ref, ref, send_sems.at[kind]).wait()

        blocks = 3 if is_inner else 4
        sent(g.at[0, 0, :, :blocks * seq], S_GY)
        sent(act.at[0, :blocks], S_PY)
        sent(g.at[:, :, :, seq:], S_GX)
        sent(pa.at[1:], S_PX)
        sent(binv.at[:15 * seq, :], S_ACT)
        sent(bt.at[:, :3 * chunk, :], S_BT)
        sent(rsb.at[:, :7], S_RS)
        sent(rsb.at[:, :7], S_AG)
        sent(xrecv, S_OC)
        sent(yrecv, S_OY)

    at(999, 999, drain)
    assert counter[0] == recv_sems.shape[0]
    for _, _, fn in sorted(steps, key=lambda s: (s[0], s[1])):
        fn()


def shards(activations, gradients, basis_in, basis_out):
    seq, feat = gradients.shape[1:]
    cols = basis_out.shape[1]
    width = basis_in.shape[1]
    half = (cols + 31) // 32 * 32
    chunk = half // 2
    gt = gradients[0].T
    dims = (feat, seq, half, chunk, width)
    return pl.pallas_call(
        functools.partial(kernel, dims),
        out_shape=jax.ShapeDtypeStruct((cols, width), F32),
        in_specs=[pl.BlockSpec(memory_space=pltpu.HBM)] * 4,
        out_specs=pl.BlockSpec(memory_space=pltpu.VMEM),
        scratch_shapes=[
            pltpu.VMEM((feat, cols), BF16),
            pltpu.VMEM((NYL, 2 * half, feat), BF16),
            pltpu.VMEM((feat, seq), BF16),
            pltpu.VMEM((2, NYL, feat, 4 * seq), BF16),
            pltpu.VMEM((NYL, NZ, seq, width), BF16),
            pltpu.VMEM(basis_in.shape, BF16),
            pltpu.VMEM((seq, width), BF16),
            pltpu.VMEM((4, 2 * seq, 2 * width), BF16),
            pltpu.VMEM((4, NZ, chunk, seq), BF16),
            pltpu.VMEM((4, NZ, chunk, seq), BF16),
            pltpu.VMEM((4, NZ * chunk, seq), BF16),
            pltpu.VMEM((2 * half, 2 * width), F32),
            pltpu.VMEM((half, 2 * width), F32),
            pltpu.VMEM((half, width), BF16),
            pltpu.VMEM((half, width), BF16),
            pltpu.SemaphoreType.DMA((10,)),
            pltpu.SemaphoreType.DMA((145,)),
            pltpu.SemaphoreType.DMA((5,)),
        ],
        compiler_params=pltpu.CompilerParams(
            collective_id=0, has_side_effects=True, vmem_limit_bytes=40 * 1024 * 1024
        ),
        name="ekfac",
    )(*[pltpu.with_memory_space_constraint(v, pltpu.HBM) for v in (basis_out, gt, activations[0], basis_in)])


def solution(mesh):
    return jax.shard_map(
        shards,
        mesh=mesh,
        in_specs=(P("dp", None, "mp"), P("dp", None, "mp"), P(None, "mp"), P("mp", "dp")),
        out_specs=P("dp", "mp"),
        check_vma=False,
    )
```

```python
import functools

import jax
import jax.numpy as jnp
from jax import lax
from jax.experimental import pallas as pl
from jax.experimental.pallas import tpu as pltpu
from jax.sharding import PartitionSpec as P

MESH = pl.DeviceIdType.MESH
NX, NYH, NYL, NZ = 4, 4, 2, 8
F32, BF16 = jnp.float32, jnp.bfloat16
SETS = (((0, 0), (1, 0), (2, 0), (0, 1)), ((3, 0), (1, 1), (2, 1), (3, 1)))
HOME = {key: (k, pos) for k, keys in enumerate(SETS) for pos, key in enumerate(keys)}


def kernel(
    dims, basis_hbm, gt_hbm, act_hbm, bin_hbm, out_ref,
    raw, bt, gt, g, act, binv, paloc, pa, part, rsb, pg, acc, xrecv, ysend, yrecv,
    send_sems, recv_sems, loc_sems,
):
    feat, seq, half, chunk, width = dims
    dp, mp = lax.axis_index("dp"), lax.axis_index("mp")
    core, x, yh = dp % 2, (dp // 2) % NX, dp // (2 * NX)
    yl, z = mp // NZ, mp % NZ

    def dev(yh_=None, x_=None, c_=None, yl_=None, z_=None):
        yh_ = yh if yh_ is None else yh_
        x_ = x if x_ is None else x_
        c_ = core if c_ is None else c_
        yl_ = yl if yl_ is None else yl_
        z_ = z if z_ is None else z_
        return ((yh_ * NX + x_) * 2 + c_, yl_ * NZ + z_)

    sibling = dev(c_=1 - core)
    ypart = dev(yl_=1 - yl)
    xn = {1: dev(x_=(x + 1) % NX), -1: dev(x_=(x + NX - 1) % NX)}
    zn = {k: dev(z_=(z + NZ + k) % NZ) for k in (1, -1, 2, -2)}

    y = yh * NYL + yl
    ny = NYH * NYL

    def ydev(k):
        yy = (y + ny + k) % ny
        return dev(yh_=yy // NYL, yl_=yy % NYL)

    sigma = 1 - 2 * (yh % 2)
    inner = yl == yh % 2
    outer = yl != yh % 2

    def own_block():
        return g.at[0, 0, :, :seq]

    barrier = pltpu.get_barrier_semaphore()
    peers = [ydev(2), ydev(-2), zn[2], zn[-2], ydev(1), ydev(-1), xn[1], xn[-1], zn[1], zn[-1], sibling]
    for peer in peers:
        pl.semaphore_signal(barrier, inc=1, device_id=peer, device_id_type=MESH)
    pltpu.make_async_copy(gt_hbm, gt, loc_sems.at[0]).start()
    pltpu.make_async_copy(act_hbm, act.at[0, z], loc_sems.at[1]).start()
    pltpu.make_async_copy(basis_hbm, raw, loc_sems.at[4]).start()
    pltpu.make_async_copy(bin_hbm, binv, loc_sems.at[2]).start()
    pl.when(inner)(lambda: pltpu.make_async_copy(gt_hbm, own_block(), loc_sems.at[3]).start())
    pl.semaphore_wait(barrier, len(peers))

    refs = (basis_hbm, gt_hbm, act_hbm, bin_hbm, out_ref, raw, bt, gt, g, act, binv, paloc, pa, part, rsb, pg, acc,
            xrecv, ysend, yrecv, send_sems, recv_sems, loc_sems)
    where = (core, yl, z, sigma, sibling, ypart, xn, zn, ydev, own_block)
    pl.when(inner)(lambda: program(True, dims, where, *refs))
    pl.when(outer)(lambda: program(False, dims, where, *refs))


def program(
    is_inner, dims, where, basis_hbm, gt_hbm, act_hbm, bin_hbm, out_ref, raw, bt, gt, g, act, binv, paloc, pa, part,
    rsb, pg, acc, xrecv, ysend, yrecv, send_sems, recv_sems, loc_sems,
):
    feat, seq, half, chunk, width = dims
    core, yl, z, sigma, sibling, ypart, xn, zn, ydev, own_block = where
    counter = [0]

    def take(n=1):
        base = counter[0]
        counter[0] += n
        return base

    S_GY, S_GX, S_PY, S_PX, S_ACT, S_BT, S_RS, S_AG, S_OC, S_OY = range(10)

    def send(src, dst, kind, rsem, to):
        pltpu.make_async_remote_copy(
            src_ref=src, dst_ref=dst, send_sem=send_sems.at[kind], recv_sem=recv_sems.at[rsem],
            device_id=to, device_id_type=MESH,
        ).start()

    def arrived(dst, rsem):
        pltpu.make_async_copy(dst, dst, recv_sems.at[rsem]).wait()

    s_bt = take(6)
    s_act0 = take(1)
    s_gy, s_gx = take(8), take(24)
    s_py, s_px = take(8), take(12)
    s_actz = take(16)
    s_rs, s_ag = take(32), take(32)
    s_out = take(6)

    def num(part):
        return 1 if part == 1 else 0

    def y_start(pat):
        place, source, parts, base, _, kind, _ = pat

        def from_outer():
            for p in parts:
                for d in (1, -1):
                    send(source(p), place(0, 0, 1, p), kind, base + num(p), ydev(d))

        def from_inner():
            for p in parts:
                send(source(p), place(0, 0, 0, p), kind, base + 2 + num(p), ydev(2 * sigma))
                for h in (0, 1) if p is None else (p,):
                    send(source(h), place(0, 1, 0, h), kind, base + 6 + h, ydev(-2 * sigma))

        from_inner() if is_inner else from_outer()

    def x_send(pat, a, f, p):
        place, _, parts, _, base, _, kind = pat
        for d, slot in ((1, 1), (-1, 2)):
            s = base + ((slot - 1) * 4 + a * 2 + f) * len(parts) + num(p)
            send(place(0, a, f, p), place(slot, a, f, p), kind, s, xn[d])

    def y_near_other(pat, p):
        place, _, _, base, _, kind, _ = pat
        arrived(place(0, 0, 1, p), base + num(p))
        send(place(0, 0, 1, p), place(0, 1, 1, p), kind, base + 4 + num(p), ydev(-2 * sigma))
        x_send(pat, 0, 1, p)

    def y_near_own(pat):
        place, _, parts, base, _, kind, _ = pat
        for p in parts:
            if not is_inner:
                arrived(place(0, 0, 0, p), base + 2 + num(p))
                if p != 1:
                    send(place(0, 0, 0, 0), place(0, 1, 0, 0), kind, base + 6, ydev(-2 * sigma))
            x_send(pat, 0, 0, p)

    def y_far_own(pat):
        place, _, parts, base, _, kind, _ = pat
        for h in (1, 0):
            arrived(place(0, 1, 0, h), base + 6 + h)
            if not is_inner and h == 1:
                send(place(0, 1, 0, 1), place(0, 1, 0, 1), kind, base + 7, ydev(2 * sigma))
            if h in parts:
                x_send(pat, 1, 0, h)
        if None in parts:
            x_send(pat, 1, 0, None)

    def y_far_other(pat, p):
        place, _, _, base, _, _, _ = pat
        arrived(place(0, 1, 1, p), base + 4 + num(p))
        x_send(pat, 1, 1, p)

    def x_near(pat, a, f):
        place, _, parts, _, base, _, kind = pat
        for p in parts:
            for d, slot in ((1, 1), (-1, 2)):
                s = base + ((slot - 1) * 4 + a * 2 + f) * len(parts) + num(p)
                arrived(place(slot, a, f, p), s)
                if f == slot - 1:
                    s = base + (8 + a * 2 + f) * len(parts) + num(p)
                    send(place(slot, a, f, p), place(3, a, f, p), kind, s, xn[d])

    def x_far(pat, a, f):
        place, _, parts, _, base, _, _ = pat
        for p in parts:
            arrived(place(3, a, f, p), base + (8 + a * 2 + f) * len(parts) + num(p))

    cut = (feat // 2 + 15) // 16 * 16
    g_parts = {None: slice(None), 0: slice(0, cut), 1: slice(cut, feat)}
    p_parts = {None: (0, seq), 0: (0, seq // 2), 1: (seq // 2, seq)}

    def g_place(slot, a, f, part_=None):
        k, pos = HOME[slot, a]
        return g.at[k, f, g_parts[part_], pos * seq:(pos + 1) * seq]

    def p_place(slot, a, f, part_=None):
        lo, hi = p_parts[part_]
        return pa.at[slot, a * seq + lo:a * seq + hi, f * width:(f + 1) * width]

    def g_source(p):
        return gt.at[g_parts[p], :]

    def p_source(p):
        return paloc.at[slice(*p_parts[p]), :]

    gpat = (g_place, g_source, (0, 1), s_gy, s_gx, S_GY, S_GX)
    ppat = (p_place, p_source, (None,), s_py, s_px, S_PY, S_PX)

    def bt_place(f, c, i):
        return bt.at[f, pl.ds(pl.multiple_of(c * half + i * chunk, 16), chunk), :]

    def start():
        pltpu.make_async_copy(gt_hbm, gt, loc_sems.at[0]).wait()
        y_start(gpat)
        pltpu.make_async_copy(act_hbm, act.at[0, z], loc_sems.at[1]).wait()
        send(act.at[0, z], act.at[1, z], S_ACT, s_act0, ypart)

    def g_own():
        if is_inner:
            pltpu.make_async_copy(gt_hbm, own_block(), loc_sems.at[3]).wait()
        y_near_own(gpat)

    def bt_own():
        pltpu.make_async_copy(basis_hbm, raw, loc_sems.at[4]).wait()
        turned = raw[...].T
        bt[0, pl.ds(pl.multiple_of(core * half, 16), turned.shape[0]), :] = turned

    def bt_rows(f, lo, hi):
        return bt.at[f, pl.ds(pl.multiple_of(core * half + lo, 16), hi - lo), :]

    def bt_send(i, pieces=(0, 1)):
        split = chunk // 32 * 16
        for lo, hi in [((0, split), (split, chunk))[piece] for piece in pieces]:
            lo, hi = i * chunk + lo, i * chunk + hi
            send(bt_rows(0, lo, hi), bt_rows(1, lo, hi), S_BT, s_bt + 2 + i, ypart)
            send(bt_rows(0, lo, hi), bt_rows(0, lo, hi), S_BT, s_bt + i, sibling)

    def bt_forward(i):
        arrived(bt_place(1, core, i), s_bt + 2 + i)
        send(bt_place(1, core, i), bt_place(1, core, i), S_BT, s_bt + 4 + i, sibling)

    def bt_ready(i):
        arrived(bt_place(0, 1 - core, i), s_bt + i)
        arrived(bt_place(1, 1 - core, i), s_bt + 4 + i)

    def act_send(f, owner, k, tag):
        send(act.at[f, owner], act.at[f, owner], S_ACT, s_actz + tag, zn[k])

    def act_tag(f, d, dist):
        return f * 8 + (0 if d == 1 else 4) + dist - 1

    def act_first(f):
        if f == 1:
            arrived(act.at[1, z], s_act0)
        for dist in (2, 1):
            for d in (1, -1):
                act_send(f, z, d * dist, act_tag(f, d, dist))

    def act_wait(f, d, dist):
        arrived(act.at[f, (z + NZ - d * dist) % NZ], s_actz + act_tag(f, d, dist))

    def act_forward():
        for f in range(2):
            for d in (1, -1):
                act_wait(f, d, 2)
                owner = (z + NZ - 2 * d) % NZ
                if (f == 0) == (d == 1):
                    act_send(f, owner, 2 * d, act_tag(f, d, 4))
                act_send(f, owner, d, act_tag(f, d, 3))

    def act_rest():
        for dist in (1, 3, 4):
            for f in range(2):
                for d in (1, -1):
                    if dist < 4 or (f == 0) == (d == 1):
                        act_wait(f, d, dist)

    def project_acts():
        pltpu.make_async_copy(bin_hbm, binv, loc_sems.at[2]).wait()
        total = None
        for f in range(2):
            low = (yl if f == 0 else 1 - yl) * NZ
            rows = pl.ds(pl.multiple_of(low * width, 128), NZ * width)
            wide = jnp.concatenate([act[f, i] for i in range(NZ)], axis=1)
            t = jnp.dot(wide, binv[rows, :], preferred_element_type=F32)
            total = t if total is None else total + t
        paloc[...] = total.astype(BF16)

        if is_inner:
            pa[0, :seq, :width] = total.astype(BF16)

    def pa_start():
        y_start(ppat)

    def project(grp):
        a, i = grp // 2, grp % 2

        def body(c, carry):
            rows = pl.ds(pl.multiple_of(c * half + i * chunk, 16), chunk)
            for pair in range(2):
                cols = slice(2 * pair * seq, 2 * (pair + 1) * seq)
                t = jnp.dot(bt[0, rows, :], g[a, 0, :, cols], preferred_element_type=F32)
                t = t + jnp.dot(bt[1, rows, :], g[a, 1, :, cols], preferred_element_type=F32)
                t = t.astype(BF16)
                part[grp, c * 4 + 2 * pair] = t[:, :seq]
                part[grp, c * 4 + 2 * pair + 1] = t[:, seq:]
            return carry

        lax.fori_loop(0, 2, body, 0)

    def rlen(grp, d):
        return 4 if (grp % 2 == 0) == (d == 1) else 3

    def rs_slot(d, k):
        return (0 if d == 1 else 4) + k

    def rs_step(grp, k):
        for d in (1, -1):
            n = rlen(grp, d)
            if k < n:
                j = (z + NZ + d * (n - k)) % NZ
                if k == 0:
                    src = part.at[grp, j]
                else:
                    slot = rs_slot(d, k - 1)
                    src = rsb.at[grp, slot]
                    arrived(src, s_rs + grp * 8 + slot)
                    rsb[grp, slot] = (rsb[grp, slot].astype(F32) + part[grp, j].astype(F32)).astype(BF16)
                s = s_rs + grp * 8 + rs_slot(d, k)
                send(src, rsb.at[grp, rs_slot(d, k)], S_RS, s, zn[d])

    def rs_two_first(grp):
        for d in (1, -1):
            for dist, hop, slot in ((4, 2, 2), (3, 1, 1), (1, 1, 0)):
                if dist <= rlen(grp, d):
                    slot = rs_slot(d, slot)
                    send(part.at[grp, (z + NZ + d * dist) % NZ], rsb.at[grp, slot], S_RS, s_rs + grp * 8 + slot, zn[d * hop])

    def rs_two_middle(grp):
        for d in (1, -1):
            total = part[grp, (z + NZ + 2 * d) % NZ].astype(F32)
            for k in range(1, rlen(grp, d) - 1):
                slot = rs_slot(d, k)
                arrived(rsb.at[grp, slot], s_rs + grp * 8 + slot)
                total = total + rsb[grp, slot].astype(F32)
            rsb[grp, rs_slot(d, 1)] = total.astype(BF16)
            slot = rs_slot(d, 3)
            send(rsb.at[grp, rs_slot(d, 1)], rsb.at[grp, slot], S_RS, s_rs + grp * 8 + slot, zn[2 * d])

    def pg_place(grp, j):
        return pg.at[grp, pl.ds(pl.multiple_of(j * chunk, 16), chunk), :]

    def ag_sem(grp, d, k):
        return s_ag + grp * 8 + rs_slot(d, k)

    def rs_last(grp, two_steps=False, ag_two_steps=False):
        total = part[grp, z].astype(F32)
        for d in (1, -1):
            for k in (0, 3) if two_steps else (rlen(grp, d) - 1,):
                slot = rs_slot(d, k)
                arrived(rsb.at[grp, slot], s_rs + grp * 8 + slot)
                total = total + rsb[grp, slot].astype(F32)
        pg[grp, pl.ds(pl.multiple_of(z * chunk, 16), chunk), :] = total.astype(BF16)
        for dist in (2, 1) if ag_two_steps else (1,):
            for d in (1, -1):
                send(pg_place(grp, z), pg_place(grp, z), S_AG, ag_sem(grp, d, dist - 1), zn[d * dist])

    def ag_wait(grp, d, dist):
        j = (z + NZ - d * dist) % NZ
        arrived(pg_place(grp, j), ag_sem(grp, d, dist - 1))
        return pg_place(grp, j)

    def ag_step(grp, k):
        for d in (1, -1):
            n = rlen(grp, d)
            if k <= n:
                piece = ag_wait(grp, d, k)
                if k < n:
                    send(piece, piece, S_AG, ag_sem(grp, d, k), zn[d])

    def ag_two_middle(grp):
        for d in (1, -1):
            piece = ag_wait(grp, d, 2)
            if rlen(grp, d) == 4:
                send(piece, piece, S_AG, ag_sem(grp, d, 3), zn[2 * d])
            send(piece, piece, S_AG, ag_sem(grp, d, 2), zn[d])

    def ag_two_last(grp):
        for dist in (1, 3, 4):
            for d in (1, -1):
                if dist <= rlen(grp, d):
                    ag_wait(grp, d, dist)

    def squares(grp, lo, hi, whose=None):
        a, i = grp // 2, grp % 2

        def body(c, carry):
            rows = pl.ds(pl.multiple_of(c * half + i * chunk, 16), chunk)
            total = None if a == 0 else acc[rows, lo:hi]
            for pos, (slot, far) in enumerate(SETS[a]):
                lhs = pg[grp, pl.ds(pl.multiple_of((c * 4 + pos) * chunk, 16), chunk), :]
                t = jnp.dot(lhs, pa[slot, far * seq:(far + 1) * seq, lo:hi], preferred_element_type=F32)
                total = t * t if total is None else total + t * t
            acc[rows, lo:hi] = total
            return carry

        if whose is None:
            lax.fori_loop(0, 2, body, 0)
        else:
            body(core if whose else 1 - core, 0)

    spans = (slice(0, width), slice(width, 2 * width))

    def acc_rows(c, i):
        return pl.ds(pl.multiple_of(c * half + i * chunk, 8), chunk)

    def out_core(i, f):
        dst = xrecv.at[i * chunk:(i + 1) * chunk, spans[f]]
        send(acc.at[acc_rows(1 - core, i), spans[f]], dst, S_OC, s_out + 2 * i + f, sibling)

    def out_y(i):
        rows = slice(i * chunk, (i + 1) * chunk)
        arrived(xrecv.at[rows, spans[1]], s_out + 2 * i + 1)
        ysend[rows, :] = (acc[acc_rows(core, i), spans[1]] + xrecv[rows, spans[1]]).astype(BF16)
        send(ysend.at[rows, :], yrecv.at[rows, :], S_OY, s_out + 4 + i, ypart)

    def out_y_of(i, c):
        pl.when(core == c)(lambda: out_y(i))

    def out_last(i):
        rows = slice(i * chunk, (i + 1) * chunk)
        n = min(chunk, out_ref.shape[0] - i * chunk)
        arrived(xrecv.at[rows, spans[0]], s_out + 2 * i)
        own = acc[acc_rows(core, i), spans[0]] + xrecv[rows, spans[0]]
        arrived(yrecv.at[rows, :], s_out + 4 + i)
        own = (own + yrecv[rows, :].astype(F32)) * (1.0 / 4096.0)
        out_ref[i * chunk:i * chunk + n, :] = own[:n]

    steps = []

    def at(t_inner, t_outer, fn, *args):
        steps.append((t_inner if is_inner else t_outer, len(steps), functools.partial(fn, *args)))

    at(0, 0, start)
    at(0.04, 11, g_own)
    at(0.05, 0.05, act_first, 0)
    at(0.3, 0.3, bt_own)
    at(0.35, 6.4, bt_send, 0, (0,))
    at(0.35, 11.2, bt_send, 0, (1,))
    at(0.36, 11.25, bt_send, 1)
    at(4, 4.5, y_near_other, gpat, 0)
    at(5.8, 6.3, y_near_other, gpat, 1)
    at(6.5, 15.5, x_near, gpat, 0, 0)
    at(15.45, 11.1, y_far_own, gpat)
    at(10.5, 12, x_near, gpat, 0, 1)
    at(11, 13, y_far_other, gpat, 0)
    at(12.5, 14.5, y_far_other, gpat, 1)
    at(12.6, 12.1, act_first, 1)
    at(15.3, 17, act_forward)
    at(15.5, 18.2, bt_forward, 0)
    at(28, 22.42, x_far, gpat, 0, 0)
    at(28, 22.42, x_far, gpat, 0, 1)
    at(15.4, 18.8, x_near, gpat, 1, 1)
    at(20.9, 18.5, x_near, gpat, 1, 0)
    at(18.5, 18.6, bt_ready, 0)
    at(18.6, 18.6, project, 0)
    at(18.6, 18.6, rs_two_first, 0)
    at(20.96, 19, rs_two_middle, 0)
    at(28.3, 28.3, rs_last, 0, True)
    for k in range(1, 5):
        at(28.9 + 3.9 * k, 28.9 + 3.9 * k, ag_step, 0, k)
    at(25.1, 22.41, act_rest)
    at(25.1, 22.41, project_acts)
    at(25.1, 22.41, pa_start)
    at(20.95, 18.7, bt_forward, 1)
    at(25, 22.4, bt_ready, 1)
    at(25, 22.4, project, 1)
    at(25, 22.4, rs_step, 1, 0)
    at(28, 28, x_far, gpat, 1, 0)
    at(28, 28, x_far, gpat, 1, 1)
    for grp in (2, 3):
        at(28 + grp / 20, 28 + grp / 20, project, grp)
        at(28 + grp / 20, 28 + grp / 20, rs_step, grp, 0)
    at(25.2, 33.46, y_near_own, ppat)
    at(33.45, 33.45, y_near_other, ppat, None)
    at(41.1, 33.47, y_far_own, ppat)
    at(41, 41, y_far_other, ppat, None)
    for i, (a, f) in enumerate(((0, 0), (0, 1), (1, 1), (1, 0))):
        t = (43, 43, 47.4, 47.4)[i]
        at(t, t, x_near, ppat, a, f)
        t = (48, 48, 54.8, 54.8)[i]
        at(t, t, x_far, ppat, a, f)
    for grp, t_in, t_out, t_last in (
        (1, (28.25, 33.5, 37.5), (28.25, 33.5, 37.5), 41),
        (2, (32, 33.4, 37.4), (32, 33.4, 37.4), 40.9),
        (3, (32.1, 34, 38), (32.1, 34, 38), 41.5),
    ):
        for k in range(3):
            at(t_in[k], t_out[k], rs_step, grp, k + 1)
        two = grp in ()
        at(t_last, t_last, rs_last, grp, False, two)
        if two:
            at(t_last + 4.9, t_last + 4.9, ag_two_middle, grp)
            at(t_last + 9.9, t_last + 9.9, ag_two_last, grp)
        else:
            for k in range(1, 5):
                at(t_last + 4 * k, t_last + 4 * k, ag_step, grp, k)
    at(53, 53, squares, 0, 0, 2 * width)
    at(56.95, 56.95, squares, 2, 0, 2 * width)
    at(56.95, 56.95, out_core, 0, 1)
    at(56.95, 56.95, out_core, 0, 0)
    at(57.1, 57.1, squares, 1, 0, 2 * width)
    at(57.05, 57.05, out_y_of, 0, 0)
    at(59, 59, squares, 3, width, 2 * width, 0)
    at(59, 59, out_core, 1, 1)
    at(59, 59, squares, 3, 0, width, 0)
    at(59, 59, out_core, 1, 0)
    at(59, 59, squares, 3, width, 2 * width, 1)
    at(59, 59, out_y_of, 0, 1)
    at(61.1, 61.1, squares, 3, 0, width, 1)
    at(61, 61, out_y, 1)
    at(62, 62, out_last, 0)
    at(63, 63, out_last, 1)

    def drain():
        def sent(ref, kind):
            pltpu.make_async_copy(ref, ref, send_sems.at[kind]).wait()

        blocks = 3 if is_inner else 4
        sent(g.at[0, 0, :, :blocks * seq], S_GY)
        sent(act.at[0, :blocks], S_PY)
        sent(g.at[:, :, :, seq:], S_GX)
        sent(pa.at[1:], S_PX)
        sent(binv.at[:15 * seq, :], S_ACT)
        sent(bt.at[:, :3 * chunk, :], S_BT)
        sent(rsb.at[:, :7], S_RS)
        sent(rsb.at[:, :7], S_AG)
        sent(xrecv, S_OC)
        sent(yrecv, S_OY)

    at(999, 999, drain)
    assert counter[0] == recv_sems.shape[0]
    for _, _, fn in sorted(steps, key=lambda s: (s[0], s[1])):
        fn()


def shards(activations, gradients, basis_in, basis_out):
    seq, feat = gradients.shape[1:]
    cols = basis_out.shape[1]
    width = basis_in.shape[1]
    half = (cols + 31) // 32 * 32
    chunk = half // 2
    gt = gradients[0].T
    dims = (feat, seq, half, chunk, width)
    return pl.pallas_call(
        functools.partial(kernel, dims),
        out_shape=jax.ShapeDtypeStruct((cols, width), F32),
        in_specs=[pl.BlockSpec(memory_space=pltpu.HBM)] * 4,
        out_specs=pl.BlockSpec(memory_space=pltpu.VMEM),
        scratch_shapes=[
            pltpu.VMEM((feat, cols), BF16),
            pltpu.VMEM((NYL, 2 * half, feat), BF16),
            pltpu.VMEM((feat, seq), BF16),
            pltpu.VMEM((2, NYL, feat, 4 * seq), BF16),
            pltpu.VMEM((NYL, NZ, seq, width), BF16),
            pltpu.VMEM(basis_in.shape, BF16),
            pltpu.VMEM((seq, width), BF16),
            pltpu.VMEM((4, 2 * seq, 2 * width), BF16),
            pltpu.VMEM((4, NZ, chunk, seq), BF16),
            pltpu.VMEM((4, NZ, chunk, seq), BF16),
            pltpu.VMEM((4, NZ * chunk, seq), BF16),
            pltpu.VMEM((2 * half, 2 * width), F32),
            pltpu.VMEM((half, 2 * width), F32),
            pltpu.VMEM((half, width), BF16),
            pltpu.VMEM((half, width), BF16),
            pltpu.SemaphoreType.DMA((10,)),
            pltpu.SemaphoreType.DMA((145,)),
            pltpu.SemaphoreType.DMA((5,)),
        ],
        compiler_params=pltpu.CompilerParams(
            collective_id=0, has_side_effects=True, vmem_limit_bytes=40 * 1024 * 1024
        ),
        name="ekfac",
    )(*[pltpu.with_memory_space_constraint(v, pltpu.HBM) for v in (basis_out, gt, activations[0], basis_in)])


def solution(mesh):
    return jax.shard_map(
        shards,
        mesh=mesh,
        in_specs=(P("dp", None, "mp"), P("dp", None, "mp"), P(None, "mp"), P("mp", "dp")),
        out_specs=P("dp", "mp"),
        check_vma=False,
    )
```
